128 devices in a mesh: grp: 4 (over y, x), row: 32 (over z, core).
Axes of the slice: x: 2, y: 2, z: 16, core: 2. Of those that a mesh axis runs over, the one named last changes fastest.
The devices are a block of a 8x8x16 slice.
Arguments:
- bin_index: int32 [262144, 10], P(('grp', 'row')), parts along dimension 0, may hold values from 0 to 32767, as said below
- pair_bin: int32 [262144, 45], P(('grp', 'row')), parts along dimension 0, may hold values from 0 to 5119, as said below
- predictor: float32 [262144], P(('grp', 'row')), parts along dimension 0, may hold values from -3 to 3
- response: float32 [262144], P(('grp', 'row')), parts along dimension 0, may hold values from 0 to 8
- marginal_basis: bfloat16 [10, 32768, 200], P(None, 'row'), may hold values from -0.1875 to 0.1875
- pair_left: int32 [45, 5120], P(None, 'row'), may hold values from 0 to 1023
- pair_right: int32 [45, 5120], P(None, 'row'), may hold values from 0 to 32767, as said below
- pair_terms: int32 [45, 2], replicated, may hold values from 0 to 9, as said below
Outputs:
- diag_blocks: float32 [40, 200, 200], P('grp'), parts along dimension 0
- cross_blocks: float32 [180, 200, 200], P('grp'), parts along dimension 0
- basis_response: float32 [40, 200], P('grp'), parts along dimension 0
The draws below stay inside these ranges and needn't reach their ends.
There are 4 independent parts, one for each index of `grp`. The reference program is written for one: setup_inputs(seed, part) draws one part's arguments, and reference() takes and returns one part's arrays. A program takes and returns all parts, laid end to end along the dimension named above; an argument that names none is the same for every part. Nothing has to cross between parts.
Inputs may be any that keep to these rules, and one draw needn't show every extreme that they name: `bin_index`: row index o of the row axis holds bins o * 1024 to (o + 1) * 1024 - 1 of every covariate. Among the 2048 rows of one device, each column names bins held by any one index o at most 128 times, and exactly 128 times for some o in every column. `pair_bin`: row index o holds bin pairs o * 160 to (o + 1) * 160 - 1 of every term pair. Among the 2048 rows of one device, each column names bin pairs held by any one index o at most 128 times, and exactly 128 times for some o in every column. `pair_right`: bin pair c = o * 160 + s names a right bin held by row index s // 5, that is a bin between (s // 5) * 1024 and (s // 5 + 1) * 1024 - 1. `pair_terms`: each row holds two smooths l < r; every unordered pair of the 10 smooths stands in exactly one row.
All inputs are finite; a program needn't handle non-finite values.
Results may differ from the reference program's by a relative error of at most 0.0032.
Values may be sent and summed in bfloat16 or wider, within the bound.
No kernel may reach another device: no remote copies, remote signals or barrier semaphores. Data moves between devices by JAX's collectives and lax.ppermute only.
A program may use at most 192 MiB of HBM per device.

```python
import jax
import jax.numpy as jnp
import numpy as np
from jax import lax

J = 10
K = 200
NB = 32768
ROWS_DEV = 2048
PB_DEV = 160
P_SIZE = 45
ROWS = 65536
NB_DEV = 1024
PB = 5120
PQ = 5
CAP = 128
N_ROW = 32


def owned_column(key, row_total, capacity, owners):
    slot_total = owners * capacity
    key_hot, key_bias, key_score, key_shuffle = jax.random.split(key, 4)
    owner_bias = jax.random.randint(key_bias, (owners,), 0, 4)
    hot_owner = jax.random.randint(key_hot, (), 0, owners)
    owner_bias = jnp.where(jnp.arange(owners) == hot_owner, -1, owner_bias)
    slot_owner = jnp.arange(slot_total) // capacity
    slot_score = (owner_bias[slot_owner] + 1) * 1024 + jax.random.randint(key_score, (slot_total,), 0, 1024)
    ranking = jnp.argsort(slot_score * slot_total + jnp.arange(slot_total), stable=True)
    picked = slot_owner[ranking[:row_total]]
    return picked[jax.random.permutation(key_shuffle, row_total)]


def draw_owned(key, per_owner, columns):

    def single(device, column):
        folded = jax.random.fold_in(jax.random.fold_in(key, device), column)
        key_owner, key_offset = jax.random.split(folded)
        owner_ids = owned_column(key_owner, ROWS_DEV, CAP, N_ROW)
        offsets = jax.random.randint(key_offset, (ROWS_DEV,), 0, per_owner)
        return owner_ids * per_owner + offsets
    devices = jnp.arange(N_ROW)
    column_ids = jnp.arange(columns)
    table = jax.vmap(jax.vmap(single, (None, 0)), (0, None))(devices, column_ids)
    return jnp.transpose(table, (0, 2, 1)).reshape(ROWS, columns).astype(jnp.int32)


def draw_bin_index(key, part):
    return draw_owned(jax.random.fold_in(key, 11), NB_DEV, J)


def draw_pair_bin(key, part):
    return draw_owned(jax.random.fold_in(key, 23), PB_DEV, P_SIZE)


def draw_pair_right(key, part):
    slots = jnp.arange(PB) % PB_DEV
    owner_ids = slots // PQ
    offsets = jax.random.randint(jax.random.fold_in(key, 37), (P_SIZE, PB), 0, NB_DEV)
    return ((owner_ids * NB_DEV)[None, :] + offsets).astype(jnp.int32)


def draw_pair_terms(key, part):
    first, second = np.triu_indices(J, 1)
    table = jnp.stack([jnp.asarray(first), jnp.asarray(second)], axis=1).astype(jnp.int32)
    shuffled = jax.random.permutation(jax.random.fold_in(key, 41), P_SIZE)
    return table[shuffled]


def with_ends(values, key, smallest, top_value):
    dims = values.shape
    spot = [jax.random.randint(jax.random.fold_in(key, axis), (), 0, dims[axis]) for axis in range(len(dims))]
    values = values.at[tuple(spot)].set(smallest)
    longest = dims.index(max(dims))
    spot[longest] = (spot[longest] + 1) % dims[longest]
    return values.at[tuple(spot)].set(top_value)


def levels(stream_key, extent, pieces, smallest, largest):
    level = 1.0
    for dim, blocks in pieces:
        draws = jax.random.uniform(jax.random.fold_in(jax.random.fold_in(stream_key, 6), dim), (blocks,), jnp.float32, smallest / len(pieces), largest / len(pieces))
        level = level * jnp.repeat(jnp.exp(draws), extent[dim] // blocks).reshape((-1,) + (1,) * (len(extent) - 1 - dim))
    return level


def noise(stream_key, dims, spread, reach, shards=(), kind=jnp.bfloat16):
    gain = levels(stream_key, dims, shards, -0.22, 0.18) if shards else 1.0
    result = jax.random.normal(stream_key, dims, jnp.float32) * spread * gain
    return jnp.minimum(jnp.maximum(result, -reach), reach).astype(kind)


def setup_inputs(seed: int = 0, part: int = 0) -> dict:
    key_of = jax.random.split(jax.random.key(seed), 9)
    own_keys = jax.random.split(jax.random.fold_in(key_of[8], part), 9)
    return {
        "bin_index": draw_bin_index(jax.random.fold_in(jax.random.fold_in(key_of[8], part), 71), part),
        "pair_bin": draw_pair_bin(jax.random.fold_in(jax.random.fold_in(key_of[8], part), 71), part),
        "predictor": noise(own_keys[2], (ROWS,), 0.7, 3.0, ((0, 32),), jnp.float32),
        "response": jnp.clip(8.0 * jax.random.uniform(own_keys[3], (ROWS,), jnp.float32) ** levels(own_keys[3], (ROWS,), ((0, 32),), -0.2, 0.2), 0.0, 8.0),
        "marginal_basis": noise(key_of[4], (J, NB, K), 1024 ** -0.5, 0.1875, ((1, 32),)),
        "pair_left": with_ends(jax.random.randint(key_of[5], (P_SIZE, PB), 0, NB_DEV), jax.random.fold_in(key_of[5], 1), 0, NB_DEV - 1).astype(jnp.int32),
        "pair_right": draw_pair_right(jax.random.fold_in(key_of[8], 71), part),
        "pair_terms": draw_pair_terms(jax.random.fold_in(key_of[8], 71), part),
    }


def reference(bin_index, pair_bin, predictor, response, marginal_basis, pair_left, pair_right, pair_terms):
    rates = jnp.exp(predictor)
    working = rates * predictor + response - rates
    cov_ids = (bin_index + jnp.arange(J, dtype=jnp.int32)[None, :] * NB).reshape(-1)
    rate_rows = jnp.broadcast_to(rates[:, None], bin_index.shape).reshape(-1)
    work_rows = jnp.broadcast_to(working[:, None], bin_index.shape).reshape(-1)
    weight_sums = jax.ops.segment_sum(rate_rows, cov_ids, num_segments=J * NB).reshape(J, NB)
    work_sums = jax.ops.segment_sum(work_rows, cov_ids, num_segments=J * NB).reshape(J, NB)
    pair_ids = (pair_bin + jnp.arange(P_SIZE, dtype=jnp.int32)[None, :] * PB).reshape(-1)
    pair_rates = jnp.broadcast_to(rates[:, None], pair_bin.shape).reshape(-1)
    pair_sums = jax.ops.segment_sum(pair_rates, pair_ids, num_segments=P_SIZE * PB).reshape(P_SIZE, PB)

    def diag_one(term):
        basis = marginal_basis[term]
        weighted = (weight_sums[term][:, None] * basis).astype(jnp.bfloat16)
        block = jnp.dot(weighted.T, basis, preferred_element_type=jnp.float32)
        side = jnp.dot(work_sums[term].astype(jnp.bfloat16), basis, preferred_element_type=jnp.float32)
        return block, side

    diag_blocks, basis_response = lax.map(diag_one, jnp.arange(J, dtype=jnp.int32))
    flat_basis = marginal_basis.reshape(J * NB, K)
    owner_base = (jnp.arange(PB, dtype=jnp.int32) // PB_DEV) * NB_DEV

    def cross_one(pair):
        left = jnp.take(flat_basis, pair_terms[pair, 0] * NB + owner_base + pair_left[pair], axis=0)
        right = jnp.take(flat_basis, pair_terms[pair, 1] * NB + pair_right[pair], axis=0)
        weighted_left = (pair_sums[pair][:, None] * left).astype(jnp.bfloat16)
        return jnp.dot(weighted_left.T, right, preferred_element_type=jnp.float32)

    cross_blocks = lax.map(cross_one, jnp.arange(P_SIZE, dtype=jnp.int32))
    return diag_blocks, cross_blocks, basis_response
```

```python
import functools
import math

import jax
import jax.numpy as jnp
from jax import lax
from jax.experimental import pallas as pl
from jax.experimental.pallas import tpu as pltpu
from jax.sharding import PartitionSpec as P

LANES = 128
HALF = 64
UNIT = 40
VMEM_LIMIT = 60 * 1024 * 1024
f32, bf16, i32 = jnp.float32, jnp.bfloat16, jnp.int32
NT = (((1,), (1,)), ((), ()))
NN = (((1,), (0,)), ((), ()))


def up(value, step):
    return -(-value // step) * step


def dot(a, b, dims):
    return lax.dot_general(a, b, dims, preferred_element_type=f32)


def vmem():
    return pl.BlockSpec(memory_space=pltpu.VMEM)


def smem():
    return pl.BlockSpec(memory_space=pltpu.SMEM)


def params():
    return pltpu.CompilerParams(vmem_limit_bytes=VMEM_LIMIT)


def two_terms(value):
    high = value.astype(bf16)
    return high, (value - high.astype(f32)).astype(bf16)


class Plan:
    def __init__(self, devices, cluster, covs, width, bins, pairs, pair_block):
        self.devices, self.cluster = devices, cluster
        self.covs, self.width, self.bins = covs, width, bins
        self.pairs, self.pair_block = pairs, pair_block
        self.chips = devices // 2
        self.per = pair_block // devices
        self.own = -(-pairs // cluster)
        self.padded = self.own * cluster
        self.parts = bins // 256
        self.work_at = covs * bins // LANES
        self.pair_at = 2 * self.work_at
        self.rest = pair_block - LANES
        self.rest_fold = LANES // self.rest
        self.rest_at = self.pair_at + self.padded
        self.sum_rows = up(self.rest_at + -(-self.padded // self.rest_fold), 8)
        self.slot = up(self.per * self.own, 16)
        self.tails = -(-self.slot // HALF)
        self.packet = self.slot + self.slot // 2 + 8 * self.tails
        self.cuts = width // UNIT
        self.tail = width - LANES - HALF
        self.cross_blocks = self.blocks_of(self.own)
        self.diag_blocks = self.blocks_of(covs)
        self.cross_units = -(-self.cross_blocks * self.cuts // devices)
        self.diag_units = -(-self.diag_blocks * self.cuts // devices)
        self.diag_at = cluster * self.cross_units * UNIT
        self.share = self.diag_at + self.diag_units * UNIT

    def blocks_of(self, count):
        return count + -(-count // 2) + 1


def hist_kernel(plan, core_ref, bins_ref, pbins_ref, pred_ref, resp_ref, mine_ref, theirs_ref, iota_ref, own_ref, jo_ref):
    core = core_ref[0]
    rows = bins_ref.shape[1]
    iota_ref[...] = lax.broadcasted_iota(i32, iota_ref.shape, 0).astype(f32).astype(bf16)
    mine_ref[...] = jnp.zeros_like(mine_ref)
    theirs_ref[...] = jnp.zeros_like(theirs_ref)
    pred = pred_ref[...]
    rates = jnp.exp(pred)
    working = rates * pred + resp_ref[...] - rates
    rate_terms = two_terms(rates)
    work_terms = two_terms(working)
    chips, devices = plan.chips, plan.devices
    zero = jnp.zeros((), bf16)
    one = jnp.ones((), bf16)

    def place(owner):
        return ((owner & 1) ^ core) * chips + lax.shift_right_logical(owner, 1)

    def put(row, table):
        mine_ref[pl.ds(row, chips, stride=plan.sum_rows), :] = table[:chips]
        theirs_ref[pl.ds(row, chips, stride=plan.sum_rows), :] = table[chips:]

    pair_bins = pbins_ref[...]
    fifth = jnp.floor((pair_bins.astype(f32) + 0.5) * (1.0 / plan.per)).astype(i32)
    holder = lax.shift_right_logical(fifth, devices.bit_length() - 1)
    own_ref[...] = place(fifth & (devices - 1)).astype(f32).astype(bf16).astype(f32)
    jo_ref[...] = ((pair_bins - fifth * plan.per) * devices + holder).astype(f32)

    def pair_step(p, carry):
        own = own_ref[pl.ds(p, 1), :].astype(bf16)
        jo = jo_ref[pl.ds(p, 1), :].astype(bf16)
        own_hot = iota_ref[0:devices, :] == own
        left = jnp.concatenate([jnp.where(own_hot, t, zero) for t in rate_terms], axis=0)
        right = jnp.where(iota_ref[0 : plan.pair_block, :] == jo, one, zero)
        both = dot(left, right, NT)
        table = both[:devices] + both[devices:]
        put(plan.pair_at + p, table[:, :LANES])
        fold = plan.rest_fold
        line = plan.rest_at + p // fold
        at = (p % fold) * plan.rest
        lane = lax.broadcasted_iota(i32, (chips, LANES), 1)
        spread = jnp.concatenate([table[:, LANES:]] * fold, axis=1)
        keep = (lane >= at) & (lane < at + plan.rest)
        for ref, part in ((mine_ref, spread[:chips]), (theirs_ref, spread[chips:])):
            where = pl.ds(line, chips, stride=plan.sum_rows)
            ref[where, :] = jnp.where(keep, part, ref[where, :])
        return carry

    lax.fori_loop(0, plan.pairs, pair_step, 0)

    def cov_step(j, carry):
        ids = bins_ref[pl.ds(j, 1), :]
        owner = lax.shift_right_logical(ids, plan.bins.bit_length() - 1)
        offset = ids & (plan.bins - 1)
        spot = (lax.shift_right_logical(offset, 8) * devices + place(owner)).astype(f32).astype(bf16)
        low = (offset & 255).astype(f32).astype(bf16)
        spots = plan.parts * devices
        hot = iota_ref[0:spots, :] == spot
        left = jnp.concatenate([jnp.where(hot, t, zero) for t in rate_terms + work_terms], axis=0)
        right = jnp.where(iota_ref[0:256, :] == low, one, zero)
        both = dot(left, right, NT)
        for channel in range(2):
            base = 2 * channel * spots
            table = both[base : base + spots] + both[base + spots : base + 2 * spots]
            for part in range(plan.parts):
                for half in range(2):
                    put(
                        channel * plan.work_at + j * (plan.bins // LANES) + 2 * part + half,
                        table[part * devices : (part + 1) * devices, half * LANES : (half + 1) * LANES],
                    )
        return carry

    lax.fori_loop(0, plan.covs, cov_step, 0)


def histograms(plan, core, bins, pbins, pred, resp):
    rows = bins.shape[1]
    out = jax.ShapeDtypeStruct((plan.chips * plan.sum_rows, LANES), f32)
    tall = max(256, plan.parts * plan.devices, plan.pair_block)
    return pl.pallas_call(
        functools.partial(hist_kernel, plan),
        out_shape=(out, out),
        in_specs=[smem()] + [vmem()] * 4,
        out_specs=(vmem(), vmem()),
        scratch_shapes=[
            pltpu.VMEM((tall, rows), bf16),
            pltpu.VMEM(pbins.shape, f32),
            pltpu.VMEM(pbins.shape, f32),
        ],
        compiler_params=params(),
        name="histograms",
        cost_estimate=pl.CostEstimate(flops=12 * 10**9, bytes_accessed=8 * 10**6, transcendentals=rows),
    )(core, bins, pbins, pred, resp)


def pick_kernel(plan, terms_ref, left_ref, right_ref, basis_ref, out_ref, a_ref, b_ref):
    a_ref[...] = jnp.zeros_like(a_ref)
    b_ref[...] = jnp.zeros_like(b_ref)
    devices, slot = plan.devices, plan.slot
    count = plan.pair_block
    across = lax.broadcasted_iota(i32, (count, plan.bins), 1)
    lane = lax.broadcasted_iota(i32, (count, LANES), 1)
    extra = plan.width - LANES
    for i in range(plan.own):
        hot = (across == left_ref[:, i : i + 1]).astype(f32).astype(bf16)
        rows = dot(hot, basis_ref[terms_ref[i]], NT)
        right = right_ref[:, i : i + 1]
        high = lax.shift_right_logical(right, 5).astype(f32)
        low = (right & 31).astype(f32)
        end = jnp.concatenate([rows[:, LANES:], jnp.zeros((count, LANES - extra), f32)], axis=1)
        end = jnp.where(lane == extra, high, jnp.where(lane == extra + 1, low, end))
        for j in range(plan.per):
            where = pl.ds(j * plan.own + i, devices, stride=slot)
            a_ref[where, :] = rows[j * devices : (j + 1) * devices, :LANES]
            b_ref[where, :] = end[j * devices : (j + 1) * devices]

    def pack(q, carry):
        at = pl.multiple_of(q * slot, slot)
        a = a_ref[pl.ds(at, slot), :]
        b = b_ref[pl.ds(at, slot), :]
        half = slot // 2
        fold_lane = lax.broadcasted_iota(i32, (half, LANES), 1)
        folded = jnp.where(fold_lane < HALF, b[:half], pltpu.roll(b[half:], HALF, 1))
        tail_lane = lax.broadcasted_iota(i32, (8, LANES), 1)
        tails = []
        for n in range(plan.tails):
            tile = jnp.zeros((8, LANES), f32)
            for t in range(8):
                row = n * HALF + 8 * t
                if row >= slot:
                    break
                moved = pltpu.roll(b[row : row + 8], (16 * t - HALF) % LANES, 1)
                tile = jnp.where((tail_lane >= 16 * t) & (tail_lane < 16 * t + 16), moved, tile)
            tails.append(tile)
        out_ref[q] = jnp.concatenate([a, folded] + tails, axis=0).astype(bf16)
        return carry

    lax.fori_loop(0, devices, pack, 0)


def picked_rows(plan, terms, left, right, basis):
    return pl.pallas_call(
        functools.partial(pick_kernel, plan),
        out_shape=jax.ShapeDtypeStruct((plan.devices, plan.packet, LANES), bf16),
        in_specs=[smem()] + [vmem()] * 3,
        out_specs=vmem(),
        scratch_shapes=[pltpu.VMEM((plan.devices * plan.slot, LANES), f32)] * 2,
        compiler_params=params(),
        name="picked_rows",
        cost_estimate=pl.CostEstimate(flops=10**9, bytes_accessed=6 * 10**6, transcendentals=0),
    )(terms, left, right, basis)


def product_kernel(
    plan, core_ref, terms_ref, packet_ref, pair_w_ref, cov_w_ref, work_ref, basis_ref,
    mine_ref, theirs_ref, a_ref, b_ref, sums_ref,
):
    core = core_ref[0]
    devices, slot, chips = plan.devices, plan.slot, plan.chips
    width, own = plan.width, plan.own
    sums_ref[...] = jnp.zeros_like(sums_ref)
    half = slot // 2

    def unpack(o, carry):
        at = pl.multiple_of(o * slot, slot)
        y = packet_ref[o].astype(f32)
        a_ref[pl.ds(at, slot), :] = y[:slot]
        folded = y[slot : slot + half]
        turned = pltpu.roll(folded, HALF, 1)
        lane = lax.broadcasted_iota(i32, (8, LANES), 1)
        for n in range(plan.tails):
            tile = y[slot + half + 8 * n : slot + half + 8 * n + 8]
            for t in range(8):
                row = n * HALF + 8 * t
                if row >= slot:
                    break
                top = folded[row : row + 8] if row < half else turned[row - half : row - half + 8]
                moved = pltpu.roll(tile, (HALF - 16 * t) % LANES, 1)
                b_ref[pl.ds(at + row, 8), :] = jnp.where(lane < HALF, top, moved)
        return carry

    lax.fori_loop(0, devices, unpack, 0)

    def spot(block, cut, units, base):
        unit = block * plan.cuts + cut
        owner = unit // units
        place = ((owner & 1) ^ core) * chips + lax.shift_right_logical(owner, 1)
        return pl.multiple_of(place * plan.share + base + (unit % units) * UNIT, 8)

    def put(block, value, units, base, first=None, last=None):
        for cut in range(plan.cuts):
            where = pl.ds(spot(block, cut, units, base), UNIT)
            piece = value[cut * UNIT : (cut + 1) * UNIT]
            if first is None:
                sums_ref[where, :] = piece
            else:
                lane = lax.broadcasted_iota(i32, (UNIT, LANES), 1)
                keep = (lane >= first) & (lane < last)
                sums_ref[where, :] = jnp.where(keep, piece, sums_ref[where, :])

    def put_square(n, count, square, units, base):
        put(n, square[:, :LANES], units, base)
        rest = width - LANES
        side = jnp.concatenate([square[:, LANES:], jnp.zeros((width, LANES - rest), f32)], axis=1)
        at = (n % 2) * HALF
        put(count + n // 2, pltpu.roll(side, at, 1), units, base, at, at + HALF)
        tail_at = n * plan.tail
        put(
            count + -(-count // 2),
            pltpu.roll(side, (tail_at + HALF) % LANES, 1),
            units, base, tail_at, tail_at + plan.tail,
        )

    def diag_step(j, carry):
        basis = basis_ref[j]
        weighted = (basis.astype(f32) * cov_w_ref[pl.ds(j, 1), :]).astype(bf16)
        square = dot(weighted, basis, NT)
        put_square(j, plan.covs, square, plan.diag_units, plan.diag_at)
        side = dot(basis, work_ref[...], NT)
        column = lax.broadcasted_iota(i32, (width, LANES), 1)
        at = plan.covs * plan.tail
        put(
            plan.covs + -(-plan.covs // 2),
            pltpu.roll(side, at, 1),
            plan.diag_units, plan.diag_at, at + j, at + j + 1,
        )
        return carry

    lax.fori_loop(0, plan.covs, diag_step, 0)

    across = lax.broadcasted_iota(i32, (plan.pair_block, plan.bins), 1)
    extra = width - LANES

    def pair_step(i, carry):
        stride = [pl.ds(j * own + i, devices, stride=slot) for j in range(plan.per)]
        a = jnp.concatenate([a_ref[s, :] for s in stride], axis=0)
        b = jnp.concatenate([b_ref[s, :] for s in stride], axis=0)
        index = (b[:, extra : extra + 1] * 32.0 + b[:, extra + 1 : extra + 2]).astype(i32)
        hot = (across == index).astype(f32).astype(bf16)
        right = dot(hot, basis_ref[terms_ref[i]], NT).astype(bf16)
        left = jnp.concatenate([jnp.transpose(a), jnp.transpose(b)[:extra]], axis=0)
        for m in range(plan.cluster):
            weight = pair_w_ref[pl.ds(m * own + i, 1), :]
            square = dot((left * weight).astype(bf16), right, NN)
            put_square(i, own, square, plan.cross_units, m * plan.cross_units * UNIT)
        return carry

    lax.fori_loop(0, own, pair_step, 0)
    mine_ref[...] = sums_ref[: chips * plan.share, :]
    theirs_ref[...] = sums_ref[chips * plan.share :, :]


def products(plan, core, terms, packets, pair_w, cov_w, work, basis):
    out = jax.ShapeDtypeStruct((plan.chips * plan.share, LANES), f32)
    return pl.pallas_call(
        functools.partial(product_kernel, plan),
        out_shape=(out, out),
        in_specs=[smem(), smem()] + [vmem()] * 5,
        out_specs=(vmem(), vmem()),
        scratch_shapes=[pltpu.VMEM((plan.devices * plan.slot, LANES), f32)] * 2
        + [pltpu.VMEM((2 * plan.chips * plan.share, LANES), f32)],
        compiler_params=params(),
        name="products",
        cost_estimate=pl.CostEstimate(flops=4 * 10**9, bytes_accessed=26 * 10**6, transcendentals=0),
    )(core, terms, packets, pair_w, cov_w, work, basis)


def unpack_kernel(plan, own, count, units, base, in_ref, out_ref):
    p = pl.program_id(0)
    member, n = p // own, p % own
    start = base + member * units * UNIT

    def block(b):
        pieces = []
        for cut in range(plan.cuts):
            unit = b * plan.cuts + cut
            row = pl.multiple_of(start + (unit % units) * UNIT, 8)
            pieces.append(in_ref[unit // units, pl.ds(row, UNIT), :])
        return jnp.concatenate(pieces, axis=0).astype(f32)

    width = plan.width
    side = block(count + n // 2)
    tail = block(count + -(-count // 2))
    lane = lax.broadcasted_iota(i32, (width, LANES), 1)
    side = pltpu.roll(side, (n % 2) * HALF, 1)
    tail = pltpu.roll(tail, (HALF - n * plan.tail) % LANES, 1)
    out_ref[0, :, :LANES] = block(n)
    out_ref[0, :, LANES:] = jnp.where(lane < HALF, side, tail)[:, : width - LANES]


def unpacked(plan, total, own, count, units, base, lines):
    width = plan.width
    return pl.pallas_call(
        functools.partial(unpack_kernel, plan, own, count, units, base),
        out_shape=jax.ShapeDtypeStruct((total, width, width), f32),
        grid=(total,),
        in_specs=[vmem()],
        out_specs=pl.BlockSpec((1, width, width), lambda p: (p, 0, 0)),
        compiler_params=params(),
        name="unpacked",
        cost_estimate=pl.CostEstimate(flops=10**6, bytes_accessed=14 * 10**6, transcendentals=0),
    )(lines)


def clusters_of(groups):
    side = math.isqrt(groups)
    if side * side == groups and side % 2 == 0:
        return [
            [(y + b) * side + x + a for b in range(2) for a in range(2)]
            for y in range(0, side, 2)
            for x in range(0, side, 2)
        ]
    return [[g] for g in range(groups)]


def place_in(clusters, group):
    table = [0] * sum(len(c) for c in clusters)
    for members in clusters:
        for place, g in enumerate(members):
            table[g] = place
    return jnp.asarray(table, i32)[group]


def on_device(
    bin_index, pair_bin, predictor, response, marginal_basis, pair_left, pair_right, pair_terms
):
    devices, groups = lax.axis_size("row"), lax.axis_size("grp")
    clusters = clusters_of(groups)
    cluster = len(clusters[0])
    covs, bins, width = marginal_basis.shape
    pairs, pair_block = pair_left.shape
    plan = Plan(devices, cluster, covs, width, bins, pairs, pair_block)
    rings = [list(range(c, devices, 2)) for c in range(2)]
    swap = [(d, d ^ 1) for d in range(devices)]
    me = lax.axis_index("row")
    core = (me % 2).astype(i32).reshape(1)
    place = place_in(clusters, lax.axis_index("grp"))
    basis = jnp.swapaxes(marginal_basis, 1, 2)

    mine, theirs = histograms(
        plan, core, jnp.transpose(bin_index), jnp.transpose(pair_bin),
        predictor.reshape(1, -1), response.reshape(1, -1),
    )
    sums = mine + lax.ppermute(theirs, "row", swap)
    sums = lax.psum_scatter(sums, "row", axis_index_groups=rings, tiled=True)

    def my_pairs(table):
        padded = jnp.pad(table, ((0, plan.padded - pairs), (0, 0)))
        return lax.dynamic_slice(padded, (place * plan.own, 0), (plan.own, table.shape[1]))

    def columns(table):
        blocks = my_pairs(table).reshape(plan.own, devices, plan.per)
        return jnp.transpose(blocks, (2, 1, 0)).reshape(pair_block, plan.own)

    terms = my_pairs(pair_terms)
    packets = picked_rows(plan, terms[:, 0], columns(pair_left), columns(pair_right % bins), basis)
    packets = lax.all_to_all(packets, "row", split_axis=0, concat_axis=0, tiled=True)

    cov_w = sums[: plan.work_at].reshape(covs, bins)
    work = sums[plan.work_at : plan.pair_at].reshape(covs, bins).astype(bf16)
    work = jnp.pad(work, ((0, LANES - covs), (0, 0)))
    rest = sums[plan.rest_at : plan.rest_at + -(-plan.padded // plan.rest_fold)]
    pair_w = jnp.concatenate(
        [
            sums[plan.pair_at : plan.pair_at + plan.padded],
            rest.reshape(-1, plan.rest)[: plan.padded],
        ],
        axis=1,
    )
    if cluster > 1:
        pair_w = lax.all_to_all(
            pair_w.reshape(cluster, plan.own, pair_block), "grp", 0, 0,
            axis_index_groups=clusters, tiled=True,
        ).reshape(plan.padded, pair_block)

    mine, theirs = products(plan, core, terms[:, 1], packets, pair_w, cov_w, work, basis)
    total = mine + lax.ppermute(theirs, "row", swap)
    total = lax.psum_scatter(total, "row", axis_index_groups=rings, tiled=True)
    total = lax.optimization_barrier(total).astype(bf16)
    cross = total[: plan.diag_at]
    if cluster > 1:
        cross = lax.all_to_all(
            cross.reshape(cluster, -1, LANES), "grp", 0, 0, axis_index_groups=clusters, tiled=True
        ).reshape(plan.diag_at, LANES)
    share = jnp.concatenate([cross, total[plan.diag_at :]], axis=0)
    lines = lax.all_gather(share, "row", axis=0, tiled=True).reshape(devices, plan.share, LANES)

    cross_blocks = unpacked(plan, pairs, plan.own, plan.own, plan.cross_units, 0, lines)
    diag_blocks = unpacked(plan, covs, covs, covs, plan.diag_units, plan.diag_at, lines)
    side = []
    for cut in range(plan.cuts):
        unit = (plan.diag_blocks - 1) * plan.cuts + cut
        row = plan.diag_at + (unit % plan.diag_units) * UNIT
        side.append(lines[unit // plan.diag_units, row : row + UNIT])
    at = covs * plan.tail
    basis_response = jnp.transpose(jnp.concatenate(side, axis=0)[:, at : at + covs]).astype(f32)
    return diag_blocks, cross_blocks, basis_response


def solution(mesh):
    return jax.shard_map(
        on_device,
        mesh=mesh,
        in_specs=(
            P(("grp", "row"), None),
            P(("grp", "row"), None),
            P(("grp", "row")),
            P(("grp", "row")),
            P(None, "row", None),
            P(None, "row"),
            P(None, "row"),
            P(),
        ),
        out_specs=(P("grp", None, None), P("grp", None, None), P("grp", None)),
        check_vma=False,
    )
```

```python
import functools
import math

import jax
import jax.numpy as jnp
from jax import lax
from jax.experimental import pallas as pl
from jax.experimental.pallas import tpu as pltpu
from jax.sharding import PartitionSpec as P

LANES = 128
HALF = 64
UNIT = 40
VMEM_LIMIT = 60 * 1024 * 1024
f32, bf16, i32 = jnp.float32, jnp.bfloat16, jnp.int32
NT = (((1,), (1,)), ((), ()))
NN = (((1,), (0,)), ((), ()))


def up(value, step):
    return -(-value // step) * step


def dot(a, b, dims):
    return lax.dot_general(a, b, dims, preferred_element_type=f32)


def vmem():
    return pl.BlockSpec(memory_space=pltpu.VMEM)


def smem():
    return pl.BlockSpec(memory_space=pltpu.SMEM)


def params():
    return pltpu.CompilerParams(vmem_limit_bytes=VMEM_LIMIT)


def two_terms(value):
    high = value.astype(bf16)
    return high, (value - high.astype(f32)).astype(bf16)


class Plan:
    def __init__(self, devices, cluster, covs, width, bins, pairs, pair_block):
        self.devices, self.cluster = devices, cluster
        self.covs, self.width, self.bins = covs, width, bins
        self.pairs, self.pair_block = pairs, pair_block
        self.chips = devices // 2
        self.per = pair_block // devices
        self.own = -(-pairs // cluster)
        self.padded = self.own * cluster
        self.parts = bins // 256
        self.work_at = covs * bins // LANES
        self.pair_at = 2 * self.work_at
        self.rest = pair_block - LANES
        self.rest_fold = LANES // self.rest
        self.member = up(self.own + -(-self.own // self.rest_fold), 8)
        self.sum_rows = up(self.pair_at + self.cluster * self.member, 8)
        self.slot = up(self.per * self.own, 16)
        self.tails = -(-self.slot // HALF)
        self.packet = self.slot + self.slot // 2 + 8 * self.tails
        self.cuts = width // UNIT
        self.tail = width - LANES - HALF
        self.cross_blocks = self.blocks_of(self.own)
        self.diag_blocks = self.blocks_of(covs)
        self.cross_units = -(-self.cross_blocks * self.cuts // devices)
        self.diag_units = -(-self.diag_blocks * self.cuts // devices)
        self.diag_at = cluster * self.cross_units * UNIT
        self.share = self.diag_at + self.diag_units * UNIT
        self.starts = [m * self.cross_units * UNIT for m in range(cluster)] + [self.diag_at]
        self.counts = [self.cross_units * UNIT] * cluster + [self.diag_units * UNIT]
        self.chunk = up(max(c + c // UNIT for c in self.counts), 16)

    def blocks_of(self, count):
        return count + -(-count // 2) + 1


def hist_kernel(plan, core_ref, bins_ref, pbins_ref, pred_ref, resp_ref, mine_ref, theirs_ref, iota_ref, own_ref, jo_ref):
    core = core_ref[0]
    rows = bins_ref.shape[1]
    iota_ref[...] = lax.broadcasted_iota(i32, iota_ref.shape, 0).astype(f32).astype(bf16)
    mine_ref[...] = jnp.zeros_like(mine_ref)
    theirs_ref[...] = jnp.zeros_like(theirs_ref)
    pred = pred_ref[...]
    rates = jnp.exp(pred)
    working = rates * pred + resp_ref[...] - rates
    rate_terms = two_terms(rates)
    work_terms = two_terms(working)
    chips, devices = plan.chips, plan.devices
    zero = jnp.zeros((), bf16)
    one = jnp.ones((), bf16)

    def place(owner):
        return ((owner & 1) ^ core) * chips + lax.shift_right_logical(owner, 1)

    def put(row, table):
        mine_ref[pl.ds(row, chips, stride=plan.sum_rows), :] = table[:chips]
        theirs_ref[pl.ds(row, chips, stride=plan.sum_rows), :] = table[chips:]

    middle = plan.pair_block // 2
    pair_bins = pbins_ref[...]
    fifth = jnp.floor((pair_bins.astype(f32) + 0.5) * (1.0 / plan.per)).astype(i32)
    holder = lax.shift_right_logical(fifth, devices.bit_length() - 1)
    within = (pair_bins - fifth * plan.per) * devices + holder
    late = (within >= middle).astype(i32)
    own_ref[...] = (place(fifth & (devices - 1)) + late * devices).astype(f32)
    jo_ref[...] = (within - late * middle).astype(f32)

    def pair_step(p, carry):
        own = own_ref[pl.ds(p, 1), :].astype(bf16)
        jo = jo_ref[pl.ds(p, 1), :].astype(bf16)
        own_hot = iota_ref[0 : 2 * devices, :] == own
        left = jnp.concatenate([jnp.where(own_hot, t, zero) for t in rate_terms], axis=0)
        right = jnp.where(iota_ref[0:middle, :] == jo, one, zero)
        both = dot(left, right, NT)
        table = both[: 2 * devices] + both[2 * devices :]
        table = jnp.concatenate([table, jnp.zeros((2 * devices, LANES - middle), f32)], axis=1)
        lane = lax.broadcasted_iota(i32, (devices, LANES), 1)
        second = table[devices:]
        first_line = plan.pair_at + (p // plan.own) * plan.member
        n = p % plan.own
        put(first_line + n, jnp.where(lane < middle, table[:devices], pltpu.roll(second, middle, 1)))
        line = first_line + plan.own + n // plan.rest_fold
        at = (n % plan.rest_fold) * plan.rest
        moved = pltpu.roll(second, (at + middle) % LANES, 1)
        keep = (lane[:chips] >= at) & (lane[:chips] < at + plan.rest)
        for ref, part in ((mine_ref, moved[:chips]), (theirs_ref, moved[chips:])):
            where = pl.ds(line, chips, stride=plan.sum_rows)
            ref[where, :] = jnp.where(keep, part, ref[where, :])
        return carry

    lax.fori_loop(0, plan.pairs, pair_step, 0, unroll=3)

    def cov_step(j, carry):
        ids = bins_ref[pl.ds(j, 1), :]
        owner = lax.shift_right_logical(ids, plan.bins.bit_length() - 1)
        offset = ids & (plan.bins - 1)
        spot = (lax.shift_right_logical(offset, 8) * devices + place(owner)).astype(f32).astype(bf16)
        low = (offset & 255).astype(f32).astype(bf16)
        spots = plan.parts * devices
        hot = iota_ref[0:spots, :] == spot
        left = jnp.concatenate([jnp.where(hot, t, zero) for t in rate_terms + work_terms], axis=0)
        right = jnp.where(iota_ref[0:256, :] == low, one, zero)
        both = dot(left, right, NT)
        for channel in range(2):
            base = 2 * channel * spots
            table = both[base : base + spots] + both[base + spots : base + 2 * spots]
            for part in range(plan.parts):
                for half in range(2):
                    put(
                        channel * plan.work_at + j * (plan.bins // LANES) + 2 * part + half,
                        table[part * devices : (part + 1) * devices, half * LANES : (half + 1) * LANES],
                    )
        return carry

    lax.fori_loop(0, plan.covs, cov_step, 0, unroll=2)


def histograms(plan, core, bins, pbins, pred, resp):
    rows = bins.shape[1]
    out = jax.ShapeDtypeStruct((plan.chips * plan.sum_rows, LANES), f32)
    tall = max(256, plan.parts * plan.devices)
    return pl.pallas_call(
        functools.partial(hist_kernel, plan),
        out_shape=(out, out),
        in_specs=[smem()] + [vmem()] * 4,
        out_specs=(vmem(), vmem()),
        scratch_shapes=[
            pltpu.VMEM((tall, rows), bf16),
            pltpu.VMEM(pbins.shape, f32),
            pltpu.VMEM(pbins.shape, f32),
        ],
        compiler_params=params(),
        name="histograms",
        cost_estimate=pl.CostEstimate(flops=12 * 10**9, bytes_accessed=8 * 10**6, transcendentals=rows),
    )(core, bins, pbins, pred, resp)


def pick_kernel(plan, terms_ref, left_ref, right_ref, basis_ref, out_ref, a_ref, b_ref):
    a_ref[...] = jnp.zeros_like(a_ref)
    b_ref[...] = jnp.zeros_like(b_ref)
    devices, slot = plan.devices, plan.slot
    count = plan.pair_block
    across = lax.broadcasted_iota(i32, (count, plan.bins), 1)
    lane = lax.broadcasted_iota(i32, (count, LANES), 1)
    extra = plan.width - LANES
    for i in range(plan.own):
        hot = (across == left_ref[:, i : i + 1]).astype(f32).astype(bf16)
        rows = dot(hot, basis_ref[terms_ref[i]], NT)
        right = right_ref[:, i : i + 1]
        high = lax.shift_right_logical(right, 5).astype(f32)
        low = (right & 31).astype(f32)
        end = jnp.concatenate([rows[:, LANES:], jnp.zeros((count, LANES - extra), f32)], axis=1)
        end = jnp.where(lane == extra, high, jnp.where(lane == extra + 1, low, end))
        for j in range(plan.per):
            where = pl.ds(j * plan.own + i, devices, stride=slot)
            a_ref[where, :] = rows[j * devices : (j + 1) * devices, :LANES]
            b_ref[where, :] = end[j * devices : (j + 1) * devices]

    def pack(q, carry):
        at = pl.multiple_of(q * slot, slot)
        a = a_ref[pl.ds(at, slot), :]
        b = b_ref[pl.ds(at, slot), :]
        half = slot // 2
        fold_lane = lax.broadcasted_iota(i32, (half, LANES), 1)
        folded = jnp.where(fold_lane < HALF, b[:half], pltpu.roll(b[half:], HALF, 1))
        tail_lane = lax.broadcasted_iota(i32, (8, LANES), 1)
        tails = []
        for n in range(plan.tails):
            tile = jnp.zeros((8, LANES), f32)
            for t in range(8):
                row = n * HALF + 8 * t
                if row >= slot:
                    break
                moved = pltpu.roll(b[row : row + 8], (16 * t - HALF) % LANES, 1)
                tile = jnp.where((tail_lane >= 16 * t) & (tail_lane < 16 * t + 16), moved, tile)
            tails.append(tile)
        out_ref[q] = jnp.concatenate([a, folded] + tails, axis=0).astype(bf16)
        return carry

    lax.fori_loop(0, devices, pack, 0)


def picked_rows(plan, terms, left, right, basis):
    return pl.pallas_call(
        functools.partial(pick_kernel, plan),
        out_shape=jax.ShapeDtypeStruct((plan.devices, plan.packet, LANES), bf16),
        in_specs=[smem()] + [vmem()] * 3,
        out_specs=vmem(),
        scratch_shapes=[pltpu.VMEM((plan.devices * plan.slot, LANES), f32)] * 2,
        compiler_params=params(),
        name="picked_rows",
        cost_estimate=pl.CostEstimate(flops=10**9, bytes_accessed=6 * 10**6, transcendentals=0),
    )(terms, left, right, basis)


def product_kernel(
    plan, core_ref, terms_ref, packet_ref, pair_w_ref, weights_ref, basis_ref,
    mine_ref, theirs_ref, a_ref, b_ref, work_ref, sums_ref,
):
    core = core_ref[0]
    devices, slot, chips = plan.devices, plan.slot, plan.chips
    width, own = plan.width, plan.own
    half = slot // 2

    def unpack(o, carry):
        at = pl.multiple_of(o * slot, slot)
        y = packet_ref[o].astype(f32)
        a_ref[pl.ds(at, slot), :] = y[:slot]
        folded = y[slot : slot + half]
        turned = pltpu.roll(folded, HALF, 1)
        lane = lax.broadcasted_iota(i32, (8, LANES), 1)
        for n in range(plan.tails):
            tile = y[slot + half + 8 * n : slot + half + 8 * n + 8]
            for t in range(8):
                row = n * HALF + 8 * t
                if row >= slot:
                    break
                top = folded[row : row + 8] if row < half else turned[row - half : row - half + 8]
                moved = pltpu.roll(tile, (HALF - 16 * t) % LANES, 1)
                b_ref[pl.ds(at + row, 8), :] = jnp.where(lane < HALF, top, moved)
        return carry

    lax.fori_loop(0, devices, unpack, 0)

    def spot(block, cut, units, base):
        unit = block * plan.cuts + cut
        owner = unit // units
        place = ((owner & 1) ^ core) * chips + lax.shift_right_logical(owner, 1)
        return pl.multiple_of(place * plan.share + base + (unit % units) * UNIT, 8)

    def put(block, value, units, base, first=None, last=None):
        for cut in range(plan.cuts):
            where = pl.ds(spot(block, cut, units, base), UNIT)
            piece = value[cut * UNIT : (cut + 1) * UNIT]
            if first is None:
                sums_ref[where, :] = piece
            else:
                lane = lax.broadcasted_iota(i32, (UNIT, LANES), 1)
                keep = (lane >= first) & (lane < last)
                sums_ref[where, :] = jnp.where(keep, piece, sums_ref[where, :])

    def put_square(n, count, square, units, base):
        put(n, square[:, :LANES], units, base)
        rest = width - LANES
        side = jnp.concatenate([square[:, LANES:], jnp.zeros((width, LANES - rest), f32)], axis=1)
        at = (n % 2) * HALF
        put(count + n // 2, pltpu.roll(side, at, 1), units, base, at, at + HALF)
        tail_at = n * plan.tail
        put(
            count + -(-count // 2),
            pltpu.roll(side, (tail_at + HALF) % LANES, 1),
            units, base, tail_at, tail_at + plan.tail,
        )

    def clear(count, units, base):
        blocks = plan.blocks_of(count)
        parts = [(blocks - 1) * plan.cuts + c for c in range(plan.cuts)]
        parts += list(range(blocks * plan.cuts, units * devices))
        if count % 2:
            parts += [(blocks - 2) * plan.cuts + c for c in range(plan.cuts)]
        for unit in parts:
            where = pl.ds(spot(unit // plan.cuts, unit % plan.cuts, units, base), UNIT)
            sums_ref[where, :] = jnp.zeros((UNIT, LANES), f32)

    for m in range(plan.cluster):
        clear(own, plan.cross_units, m * plan.cross_units * UNIT)
    clear(plan.covs, plan.diag_units, plan.diag_at)

    lines = plan.bins // LANES
    work_ref[...] = jnp.zeros_like(work_ref)
    for j in range(plan.covs):
        for t in range(lines):
            row = plan.work_at + j * lines + t
            work_ref[j : j + 1, t * LANES : (t + 1) * LANES] = weights_ref[row : row + 1, :]
    work = work_ref[...].astype(bf16)
    column = lax.broadcasted_iota(i32, (width, work_ref.shape[0]), 1)

    def diag_step(j, side):
        basis = basis_ref[j]
        rows = weights_ref[pl.ds(pl.multiple_of(j * lines, lines), lines), :]
        weight = jnp.concatenate([rows[t : t + 1] for t in range(lines)], axis=1)
        weighted = (basis.astype(f32) * weight).astype(bf16)
        square = dot(weighted, basis, NT)
        put_square(j, plan.covs, square, plan.diag_units, plan.diag_at)
        return jnp.where(column == j, dot(basis, work, NT), side)

    side = lax.fori_loop(0, plan.covs, diag_step, jnp.zeros(column.shape, f32))
    at = plan.covs * plan.tail
    side = jnp.concatenate([side, jnp.zeros((width, LANES - side.shape[1]), f32)], axis=1)
    put(
        plan.diag_blocks - 1, pltpu.roll(side, at, 1),
        plan.diag_units, plan.diag_at, at, at + plan.covs,
    )

    across = lax.broadcasted_iota(i32, (plan.pair_block, plan.bins), 1)
    extra = width - LANES

    def pair_step(i, carry):
        stride = [pl.ds(j * own + i, devices, stride=slot) for j in range(plan.per)]
        a = jnp.concatenate([a_ref[s, :] for s in stride], axis=0)
        b = jnp.concatenate([b_ref[s, :] for s in stride], axis=0)
        index = (b[:, extra : extra + 1] * 32.0 + b[:, extra + 1 : extra + 2]).astype(i32)
        hot = (across == index).astype(f32).astype(bf16)
        right = dot(hot, basis_ref[terms_ref[i]], NT).astype(bf16)
        left = jnp.concatenate([jnp.transpose(a), jnp.transpose(b)[:extra]], axis=0)
        for m in range(plan.cluster):
            start = m * plan.member
            turn = (LANES - (i % plan.rest_fold) * plan.rest) % LANES
            rest = pair_w_ref[pl.ds(start + own + i // plan.rest_fold, 1), :]
            rest = pltpu.roll(jnp.broadcast_to(rest, (8, LANES)), turn, 1)[:1, : plan.rest]
            weight = jnp.concatenate([pair_w_ref[pl.ds(start + i, 1), :], rest], axis=1)
            square = dot((left * weight).astype(bf16), right, NN)
            put_square(i, own, square, plan.cross_units, m * plan.cross_units * UNIT)
        return carry

    lax.fori_loop(0, own, pair_step, 0)
    mine_ref[...] = sums_ref[: chips * plan.share, :]
    theirs_ref[...] = sums_ref[chips * plan.share :, :]


def products(plan, core, terms, packets, pair_w, weights, basis):
    out = jax.ShapeDtypeStruct((plan.chips * plan.share, LANES), f32)
    return pl.pallas_call(
        functools.partial(product_kernel, plan),
        out_shape=(out, out),
        in_specs=[smem(), smem()] + [vmem()] * 4,
        out_specs=(vmem(), vmem()),
        scratch_shapes=[pltpu.VMEM((plan.devices * plan.slot, LANES), f32)] * 2
        + [
            pltpu.VMEM((up(plan.covs, 16), plan.bins), f32),
            pltpu.VMEM((2 * plan.chips * plan.share, LANES), f32),
        ],
        compiler_params=params(),
        name="products",
        cost_estimate=pl.CostEstimate(flops=4 * 10**9, bytes_accessed=26 * 10**6, transcendentals=0),
    )(core, terms, packets, pair_w, weights, basis)


def pack_kernel(plan, in_ref, out_ref):
    for k, (start, count) in enumerate(zip(plan.starts, plan.counts)):
        rows, steps = [], []
        for at in range(start, start + count, UNIT):
            part = in_ref[at : at + UNIT, :]
            top = jnp.max(jnp.max(jnp.abs(part), axis=0, keepdims=True), axis=1, keepdims=True)
            step = jnp.ceil(jnp.log2(jnp.maximum(top, 1e-30)) - 14.98)
            rows.append(jnp.round(part * jnp.exp2(-step)))
            steps.append(jnp.broadcast_to(step, (1, LANES)))
        steps.append(jnp.zeros((plan.chunk - count - len(steps), LANES), f32))
        out_ref[k] = jnp.concatenate(rows + steps, axis=0).astype(i32).astype(jnp.int16)


def packed(plan, share):
    return pl.pallas_call(
        functools.partial(pack_kernel, plan),
        out_shape=jax.ShapeDtypeStruct((plan.cluster + 1, plan.chunk, LANES), jnp.int16),
        in_specs=[vmem()],
        out_specs=vmem(),
        compiler_params=params(),
        name="packed",
        cost_estimate=pl.CostEstimate(flops=10**6, bytes_accessed=5 * 10**5, transcendentals=16),
    )(share)


def unpack_kernel(plan, each, core_ref, mine_ref, theirs_ref, cross_ref, diag_ref, side_ref, sums_ref):
    turn = pl.program_id(0)
    core = core_ref[0]
    width, covs = plan.width, plan.covs

    @pl.when(turn == 0)
    def _():
        def chip(z, carry):
            for ref, owner in ((mine_ref, 2 * z + core), (theirs_ref, 2 * z + 1 - core)):
                for k, (start, count) in enumerate(zip(plan.starts, plan.counts)):
                    part = ref[z, k * plan.chunk : (k + 1) * plan.chunk, :].astype(i32).astype(f32)
                    steps = jnp.exp2(part[count:])
                    for u in range(count // UNIT):
                        at = u * UNIT
                        sums_ref[owner, start + at : start + at + UNIT, :] = (
                            part[at : at + UNIT] * steps[u : u + 1]
                        )
            return carry

        lax.fori_loop(0, plan.chips, chip, 0)

    def block(b, units, base):
        pieces = []
        for cut in range(plan.cuts):
            unit = b * plan.cuts + cut
            row = pl.multiple_of(base + (unit % units) * UNIT, 8)
            pieces.append(sums_ref[unit // units, pl.ds(row, UNIT), :])
        return jnp.concatenate(pieces, axis=0)

    lane = lax.broadcasted_iota(i32, (width, LANES), 1)

    def square(ref, at, n, count, units, base):
        side = pltpu.roll(block(count + n // 2, units, base), (n % 2) * HALF, 1)
        tail = block(count + -(-count // 2), units, base)
        tail = pltpu.roll(tail, (HALF + LANES - n * plan.tail) % LANES, 1)
        ref[at, :, :LANES] = block(n, units, base)
        ref[at, :, LANES:] = jnp.where(lane < HALF, side, tail)[:, : width - LANES]

    def cross_step(k, carry):
        p = turn * each[0] + k
        base = (p // plan.own) * plan.cross_units * UNIT
        square(cross_ref, k, p % plan.own, plan.own, plan.cross_units, base)
        return carry

    def diag_step(k, carry):
        square(diag_ref, k, turn * each[1] + k, covs, plan.diag_units, plan.diag_at)
        return carry

    lax.fori_loop(0, each[0], cross_step, 0)
    lax.fori_loop(0, each[1], diag_step, 0)

    @pl.when(turn == 0)
    def _():
        at = covs * plan.tail
        last = block(plan.diag_blocks - 1, plan.diag_units, plan.diag_at)
        side_ref[...] = jnp.transpose(last)[at : at + covs]


def unpacked(plan, core, mine, theirs):
    width, pairs, covs = plan.width, plan.pairs, plan.covs
    turns = math.gcd(pairs, covs)
    each = (pairs // turns, covs // turns)
    return pl.pallas_call(
        functools.partial(unpack_kernel, plan, each),
        out_shape=(
            jax.ShapeDtypeStruct((pairs, width, width), f32),
            jax.ShapeDtypeStruct((covs, width, width), f32),
            jax.ShapeDtypeStruct((covs, width), f32),
        ),
        grid=(turns,),
        in_specs=[smem(), vmem(), vmem()],
        out_specs=(
            pl.BlockSpec((each[0], width, width), lambda p: (p, 0, 0)),
            pl.BlockSpec((each[1], width, width), lambda p: (p, 0, 0)),
            pl.BlockSpec((covs, width), lambda p: (0, 0)),
        ),
        scratch_shapes=[pltpu.VMEM((plan.devices, plan.share, LANES), f32)],
        compiler_params=params(),
        name="unpacked",
        cost_estimate=pl.CostEstimate(flops=10**6, bytes_accessed=17 * 10**6, transcendentals=0),
    )(core, mine, theirs)


def clusters_of(groups):
    side = math.isqrt(groups)
    if side * side == groups and side % 2 == 0:
        return [
            [(y + b) * side + x + a for b in range(2) for a in range(2)]
            for y in range(0, side, 2)
            for x in range(0, side, 2)
        ]
    return [[g] for g in range(groups)]


def place_in(clusters, group):
    table = [0] * sum(len(c) for c in clusters)
    for members in clusters:
        for place, g in enumerate(members):
            table[g] = place
    return jnp.asarray(table, i32)[group]


def on_device(
    bin_index, pair_bin, predictor, response, marginal_basis, pair_left, pair_right, pair_terms
):
    devices, groups = lax.axis_size("row"), lax.axis_size("grp")
    clusters = clusters_of(groups)
    cluster = len(clusters[0])
    covs, bins, width = marginal_basis.shape
    pairs, pair_block = pair_left.shape
    plan = Plan(devices, cluster, covs, width, bins, pairs, pair_block)
    rings = [list(range(c, devices, 2)) for c in range(2)]
    swap = [(d, d ^ 1) for d in range(devices)]
    me = lax.axis_index("row")
    core = (me % 2).astype(i32).reshape(1)
    place = place_in(clusters, lax.axis_index("grp"))
    basis = jnp.swapaxes(marginal_basis, 1, 2)

    mine, theirs = histograms(
        plan, core, jnp.transpose(bin_index), jnp.transpose(pair_bin),
        predictor.reshape(1, -1), response.reshape(1, -1),
    )
    sums = mine + lax.ppermute(theirs, "row", swap)
    sums = lax.psum_scatter(sums, "row", axis_index_groups=rings, tiled=True)

    def my_pairs(table):
        padded = jnp.pad(table, ((0, plan.padded - pairs), (0, 0)))
        return lax.dynamic_slice(padded, (place * plan.own, 0), (plan.own, table.shape[1]))

    def columns(table):
        blocks = my_pairs(table).reshape(plan.own, devices, plan.per)
        return jnp.transpose(blocks, (2, 1, 0)).reshape(pair_block, plan.own)

    terms = my_pairs(pair_terms)
    packets = picked_rows(plan, terms[:, 0], columns(pair_left), columns(pair_right % bins), basis)
    packets = lax.all_to_all(packets, "row", split_axis=0, concat_axis=0, tiled=True)

    sums, packets = lax.optimization_barrier((sums, packets))
    pair_w = sums[plan.pair_at : plan.pair_at + cluster * plan.member]
    if cluster > 1:
        pair_w = lax.all_to_all(
            pair_w.reshape(cluster, plan.member, LANES), "grp", 0, 0,
            axis_index_groups=clusters, tiled=True,
        ).reshape(cluster * plan.member, LANES)

    mine, theirs = products(plan, core, terms[:, 1], packets, pair_w, sums, basis)
    total = mine + lax.ppermute(theirs, "row", swap)
    total = lax.psum_scatter(total, "row", axis_index_groups=rings, tiled=True)
    chunks = packed(plan, total)
    if cluster > 1:
        cross = lax.all_to_all(
            chunks[:cluster], "grp", 0, 0, axis_index_groups=clusters, tiled=True
        )
        chunks = jnp.concatenate([cross, chunks[cluster:]], axis=0)
    length = chunks.shape[0] * plan.chunk
    mine = lax.all_gather(
        chunks.reshape(length, LANES), "row", axis=0, axis_index_groups=rings, tiled=True
    )
    theirs = lax.ppermute(mine, "row", swap)
    shape = (plan.chips, length, LANES)
    cross_blocks, diag_blocks, basis_response = unpacked(
        plan, core, mine.reshape(shape), theirs.reshape(shape)
    )
    return diag_blocks, cross_blocks, basis_response


def solution(mesh):
    return jax.shard_map(
        on_device,
        mesh=mesh,
        in_specs=(
            P(("grp", "row"), None),
            P(("grp", "row"), None),
            P(("grp", "row")),
            P(("grp", "row")),
            P(None, "row", None),
            P(None, "row"),
            P(None, "row"),
            P(),
        ),
        out_specs=(P("grp", None, None), P("grp", None, None), P("grp", None)),
        check_vma=False,
    )
```

```python
import functools
import math

import jax
import jax.numpy as jnp
from jax import lax
from jax.experimental import pallas as pl
from jax.experimental.pallas import tpu as pltpu
from jax.sharding import PartitionSpec as P

LANES = 128
HALF = 64
UNIT = 40
VMEM_LIMIT = 60 * 1024 * 1024
f32, bf16, i32 = jnp.float32, jnp.bfloat16, jnp.int32
NT = (((1,), (1,)), ((), ()))
NN = (((1,), (0,)), ((), ()))


def up(value, step):
    return -(-value // step) * step


def dot(a, b, dims):
    return lax.dot_general(a, b, dims, preferred_element_type=f32)


def vmem():
    return pl.BlockSpec(memory_space=pltpu.VMEM)


def smem():
    return pl.BlockSpec(memory_space=pltpu.SMEM)


def params():
    return pltpu.CompilerParams(vmem_limit_bytes=VMEM_LIMIT)


def two_terms(value):
    high = value.astype(bf16)
    return high, (value - high.astype(f32)).astype(bf16)


class Plan:
    def __init__(self, devices, cluster, covs, width, bins, pairs, pair_block):
        self.devices, self.cluster = devices, cluster
        self.covs, self.width, self.bins = covs, width, bins
        self.pairs, self.pair_block = pairs, pair_block
        self.chips = devices // 2
        self.per = pair_block // devices
        self.own = -(-pairs // cluster)
        self.padded = self.own * cluster
        self.parts = bins // 256
        self.work_at = covs * bins // LANES
        self.pair_at = 2 * self.work_at
        self.rest = pair_block - LANES
        self.rest_fold = LANES // self.rest
        self.member = up(self.own + -(-self.own // self.rest_fold), 8)
        self.sum_rows = up(self.pair_at + self.cluster * self.member, 8)
        self.slot = up(self.per * self.own, 16)
        self.tails = -(-self.slot // HALF)
        self.packet = self.slot + self.slot // 2 + 8 * self.tails
        self.cuts = width // UNIT
        self.tail = width - LANES - HALF
        self.cross_blocks = self.blocks_of(self.own)
        self.diag_blocks = self.blocks_of(covs)
        self.cross_units = -(-self.cross_blocks * self.cuts // devices)
        self.diag_units = -(-self.diag_blocks * self.cuts // devices)
        self.diag_at = cluster * self.cross_units * UNIT
        self.share = self.diag_at + self.diag_units * UNIT
        self.starts = [m * self.cross_units * UNIT for m in range(cluster)] + [self.diag_at]
        self.counts = [self.cross_units * UNIT] * cluster + [self.diag_units * UNIT]
        self.chunk = up(max(c + c // UNIT for c in self.counts), 16)

    def blocks_of(self, count):
        return count + -(-count // 2) + 1


def hist_kernel(plan, core_ref, bins_ref, pbins_ref, pred_ref, resp_ref, mine_ref, theirs_ref, iota_ref, own_ref, jo_ref):
    core = core_ref[0]
    rows = bins_ref.shape[1]
    iota_ref[...] = lax.broadcasted_iota(i32, iota_ref.shape, 0).astype(f32).astype(bf16)
    mine_ref[...] = jnp.zeros_like(mine_ref)
    theirs_ref[...] = jnp.zeros_like(theirs_ref)
    pred = pred_ref[...]
    rates = jnp.exp(pred)
    working = rates * pred + resp_ref[...] - rates
    rate_terms = two_terms(rates)
    work_terms = two_terms(working)
    chips, devices = plan.chips, plan.devices
    zero = jnp.zeros((), bf16)
    one = jnp.ones((), bf16)

    def place(owner):
        return ((owner & 1) ^ core) * chips + lax.shift_right_logical(owner, 1)

    def put(row, table):
        mine_ref[pl.ds(row, chips, stride=plan.sum_rows), :] = table[:chips]
        theirs_ref[pl.ds(row, chips, stride=plan.sum_rows), :] = table[chips:]

    middle = plan.pair_block // 2
    pair_bins = pbins_ref[...]
    fifth = jnp.floor((pair_bins.astype(f32) + 0.5) * (1.0 / plan.per)).astype(i32)
    holder = lax.shift_right_logical(fifth, devices.bit_length() - 1)
    within = (pair_bins - fifth * plan.per) * devices + holder
    late = (within >= middle).astype(i32)
    own_ref[...] = (place(fifth & (devices - 1)) + late * devices).astype(f32)
    jo_ref[...] = (within - late * middle).astype(f32)

    def pair_step(p, carry):
        own = own_ref[pl.ds(p, 1), :].astype(bf16)
        jo = jo_ref[pl.ds(p, 1), :].astype(bf16)
        own_hot = iota_ref[0 : 2 * devices, :] == own
        left = jnp.concatenate([jnp.where(own_hot, t, zero) for t in rate_terms], axis=0)
        right = jnp.where(iota_ref[0:middle, :] == jo, one, zero)
        both = dot(left, right, NT)
        table = both[: 2 * devices] + both[2 * devices :]
        table = jnp.concatenate([table, jnp.zeros((2 * devices, LANES - middle), f32)], axis=1)
        lane = lax.broadcasted_iota(i32, (devices, LANES), 1)
        second = table[devices:]
        first_line = plan.pair_at + (p // plan.own) * plan.member
        n = p % plan.own
        put(first_line + n, jnp.where(lane < middle, table[:devices], pltpu.roll(second, middle, 1)))
        line = first_line + plan.own + n // plan.rest_fold
        at = (n % plan.rest_fold) * plan.rest
        moved = pltpu.roll(second, (at + middle) % LANES, 1)
        keep = (lane[:chips] >= at) & (lane[:chips] < at + plan.rest)
        for ref, part in ((mine_ref, moved[:chips]), (theirs_ref, moved[chips:])):
            where = pl.ds(line, chips, stride=plan.sum_rows)
            ref[where, :] = jnp.where(keep, part, ref[where, :])
        return carry

    lax.fori_loop(0, plan.pairs, pair_step, 0, unroll=3)

    def cov_step(j, carry):
        ids = bins_ref[pl.ds(j, 1), :]
        owner = lax.shift_right_logical(ids, plan.bins.bit_length() - 1)
        offset = ids & (plan.bins - 1)
        spot = (lax.shift_right_logical(offset, 8) * devices + place(owner)).astype(f32).astype(bf16)
        low = (offset & 255).astype(f32).astype(bf16)
        spots = plan.parts * devices
        hot = iota_ref[0:spots, :] == spot
        left = jnp.concatenate([jnp.where(hot, t, zero) for t in rate_terms + work_terms], axis=0)
        right = jnp.where(iota_ref[0:256, :] == low, one, zero)
        both = dot(left, right, NT)
        for channel in range(2):
            base = 2 * channel * spots
            table = both[base : base + spots] + both[base + spots : base + 2 * spots]
            for part in range(plan.parts):
                for half in range(2):
                    put(
                        channel * plan.work_at + j * (plan.bins // LANES) + 2 * part + half,
                        table[part * devices : (part + 1) * devices, half * LANES : (half + 1) * LANES],
                    )
        return carry

    lax.fori_loop(0, plan.covs, cov_step, 0, unroll=2)


def histograms(plan, core, bins, pbins, pred, resp):
    rows = bins.shape[1]
    out = jax.ShapeDtypeStruct((plan.chips * plan.sum_rows, LANES), f32)
    tall = max(256, plan.parts * plan.devices)
    return pl.pallas_call(
        functools.partial(hist_kernel, plan),
        out_shape=(out, out),
        in_specs=[smem()] + [vmem()] * 4,
        out_specs=(vmem(), vmem()),
        scratch_shapes=[
            pltpu.VMEM((tall, rows), bf16),
            pltpu.VMEM(pbins.shape, f32),
            pltpu.VMEM(pbins.shape, f32),
        ],
        compiler_params=params(),
        name="histograms",
        cost_estimate=pl.CostEstimate(flops=12 * 10**9, bytes_accessed=8 * 10**6, transcendentals=rows),
    )(core, bins, pbins, pred, resp)


def pick_kernel(plan, terms_ref, left_ref, right_ref, basis_ref, out_ref, a_ref, b_ref):
    a_ref[...] = jnp.zeros_like(a_ref)
    b_ref[...] = jnp.zeros_like(b_ref)
    devices, slot = plan.devices, plan.slot
    count = plan.pair_block
    across = lax.broadcasted_iota(i32, (count, plan.bins), 1)
    lane = lax.broadcasted_iota(i32, (count, LANES), 1)
    extra = plan.width - LANES
    for i in range(plan.own):
        hot = (across == left_ref[:, i : i + 1]).astype(f32).astype(bf16)
        rows = dot(hot, basis_ref[terms_ref[i]], NT)
        right = right_ref[:, i : i + 1]
        high = lax.shift_right_logical(right, 5).astype(f32)
        low = (right & 31).astype(f32)
        end = jnp.concatenate([rows[:, LANES:], jnp.zeros((count, LANES - extra), f32)], axis=1)
        end = jnp.where(lane == extra, high, jnp.where(lane == extra + 1, low, end))
        for j in range(plan.per):
            where = pl.ds(j * plan.own + i, devices, stride=slot)
            a_ref[where, :] = rows[j * devices : (j + 1) * devices, :LANES]
            b_ref[where, :] = end[j * devices : (j + 1) * devices]

    def pack(q, carry):
        at = pl.multiple_of(q * slot, slot)
        a = a_ref[pl.ds(at, slot), :]
        b = b_ref[pl.ds(at, slot), :]
        half = slot // 2
        fold_lane = lax.broadcasted_iota(i32, (half, LANES), 1)
        folded = jnp.where(fold_lane < HALF, b[:half], pltpu.roll(b[half:], HALF, 1))
        tail_lane = lax.broadcasted_iota(i32, (8, LANES), 1)
        tails = []
        for n in range(plan.tails):
            tile = jnp.zeros((8, LANES), f32)
            for t in range(8):
                row = n * HALF + 8 * t
                if row >= slot:
                    break
                moved = pltpu.roll(b[row : row + 8], (16 * t - HALF) % LANES, 1)
                tile = jnp.where((tail_lane >= 16 * t) & (tail_lane < 16 * t + 16), moved, tile)
            tails.append(tile)
        out_ref[q] = jnp.concatenate([a, folded] + tails, axis=0).astype(bf16)
        return carry

    lax.fori_loop(0, devices, pack, 0)


def picked_rows(plan, terms, left, right, basis):
    return pl.pallas_call(
        functools.partial(pick_kernel, plan),
        out_shape=jax.ShapeDtypeStruct((plan.devices, plan.packet, LANES), bf16),
        in_specs=[smem()] + [vmem()] * 3,
        out_specs=vmem(),
        scratch_shapes=[pltpu.VMEM((plan.devices * plan.slot, LANES), f32)] * 2,
        compiler_params=params(),
        name="picked_rows",
        cost_estimate=pl.CostEstimate(flops=10**9, bytes_accessed=6 * 10**6, transcendentals=0),
    )(terms, left, right, basis)


class Blocks:
    def __init__(self, plan, core, sums_ref, share):
        self.plan, self.core, self.sums, self.share = plan, core, sums_ref, share

    def spot(self, block, cut, units, base):
        unit = block * self.plan.cuts + cut
        owner = unit // units
        place = ((owner & 1) ^ self.core) * self.plan.chips + lax.shift_right_logical(owner, 1)
        return pl.multiple_of(place * self.share + base + (unit % units) * UNIT, 8)

    def put(self, block, value, units, base, first=None, last=None):
        for cut in range(self.plan.cuts):
            where = pl.ds(self.spot(block, cut, units, base), UNIT)
            piece = value[cut * UNIT : (cut + 1) * UNIT]
            if first is not None:
                lane = lax.broadcasted_iota(i32, (UNIT, LANES), 1)
                keep = (lane >= first) & (lane < last)
                piece = jnp.where(keep, piece, self.sums[where, :])
            self.sums[where, :] = piece

    def put_square(self, n, count, square, units, base):
        width, tail = self.plan.width, self.plan.tail
        self.put(n, square[:, :LANES], units, base)
        rest = width - LANES
        side = jnp.concatenate([square[:, LANES:], jnp.zeros((width, LANES - rest), f32)], axis=1)
        at = (n % 2) * HALF
        self.put(count + n // 2, pltpu.roll(side, at, 1), units, base, at, at + HALF)
        at = n * tail
        moved = pltpu.roll(side, (at + HALF) % LANES, 1)
        self.put(count + -(-count // 2), moved, units, base, at, at + tail)

    def clear(self, count, units, base):
        plan = self.plan
        blocks = plan.blocks_of(count)
        parts = [(blocks - 1) * plan.cuts + c for c in range(plan.cuts)]
        parts += list(range(blocks * plan.cuts, units * plan.devices))
        if count % 2:
            parts += [(blocks - 2) * plan.cuts + c for c in range(plan.cuts)]
        for unit in parts:
            where = pl.ds(self.spot(unit // plan.cuts, unit % plan.cuts, units, base), UNIT)
            self.sums[where, :] = jnp.zeros((UNIT, LANES), f32)

    def finish(self, mine_ref, theirs_ref):
        half = self.plan.chips * self.share
        mine_ref[...] = self.sums[:half, :]
        theirs_ref[...] = self.sums[half:, :]


def sums_call(plan, kernel, name, share, flops, scratch, ins, *args):
    out = jax.ShapeDtypeStruct((plan.chips * share, LANES), f32)
    return pl.pallas_call(
        kernel,
        out_shape=(out, out),
        in_specs=ins,
        out_specs=(vmem(), vmem()),
        scratch_shapes=scratch + [pltpu.VMEM((2 * plan.chips * share, LANES), f32)],
        compiler_params=params(),
        name=name,
        cost_estimate=pl.CostEstimate(flops=flops, bytes_accessed=6 * 10**6, transcendentals=0),
    )(*args)


def ready_kernel(plan, terms_ref, packet_ref, basis_ref, left_ref, right_ref, a_ref, b_ref):
    devices, slot, own = plan.devices, plan.slot, plan.own
    half = slot // 2

    def unpack(o, carry):
        at = pl.multiple_of(o * slot, slot)
        y = packet_ref[o].astype(f32)
        a_ref[pl.ds(at, slot), :] = y[:slot]
        folded = y[slot : slot + half]
        turned = pltpu.roll(folded, HALF, 1)
        lane = lax.broadcasted_iota(i32, (8, LANES), 1)
        for n in range(plan.tails):
            tile = y[slot + half + 8 * n : slot + half + 8 * n + 8]
            for t in range(8):
                row = n * HALF + 8 * t
                if row >= slot:
                    break
                top = folded[row : row + 8] if row < half else turned[row - half : row - half + 8]
                moved = pltpu.roll(tile, (HALF - 16 * t) % LANES, 1)
                b_ref[pl.ds(at + row, 8), :] = jnp.where(lane < HALF, top, moved)
        return carry

    lax.fori_loop(0, devices, unpack, 0)
    across = lax.broadcasted_iota(i32, (plan.pair_block, plan.bins), 1)
    extra = plan.width - LANES

    def pair_step(i, carry):
        stride = [pl.ds(j * own + i, devices, stride=slot) for j in range(plan.per)]
        a = jnp.concatenate([a_ref[s, :] for s in stride], axis=0)
        b = jnp.concatenate([b_ref[s, :] for s in stride], axis=0)
        index = (b[:, extra : extra + 1] * 32.0 + b[:, extra + 1 : extra + 2]).astype(i32)
        hot = (across == index).astype(f32).astype(bf16)
        right_ref[i] = dot(hot, basis_ref[terms_ref[i]], NT).astype(bf16)
        left = jnp.concatenate([jnp.transpose(a), jnp.transpose(b)[:extra]], axis=0)
        left_ref[i] = left.astype(bf16)
        return carry

    lax.fori_loop(0, own, pair_step, 0)


def ready_rows(plan, terms, packets, basis):
    own, width, block = plan.own, plan.width, plan.pair_block
    return pl.pallas_call(
        functools.partial(ready_kernel, plan),
        out_shape=(
            jax.ShapeDtypeStruct((own, width, block), bf16),
            jax.ShapeDtypeStruct((own, block, width), bf16),
        ),
        in_specs=[smem(), vmem(), vmem()],
        out_specs=(vmem(), vmem()),
        scratch_shapes=[pltpu.VMEM((plan.devices * plan.slot, LANES), f32)] * 2,
        compiler_params=params(),
        name="ready_rows",
        cost_estimate=pl.CostEstimate(flops=10**9, bytes_accessed=7 * 10**6, transcendentals=0),
    )(terms, packets, basis)


def diag_kernel(plan, core_ref, weights_ref, basis_ref, mine_ref, theirs_ref, work_ref, sums_ref):
    width, units = plan.width, plan.diag_units
    blocks = Blocks(plan, core_ref[0], sums_ref, units * UNIT)
    blocks.clear(plan.covs, units, 0)
    lines = plan.bins // LANES
    work_ref[...] = jnp.zeros_like(work_ref)
    for j in range(plan.covs):
        for t in range(lines):
            row = plan.work_at + j * lines + t
            work_ref[j : j + 1, t * LANES : (t + 1) * LANES] = weights_ref[row : row + 1, :]
    work = work_ref[...].astype(bf16)
    column = lax.broadcasted_iota(i32, (width, work_ref.shape[0]), 1)

    def diag_step(j, side):
        basis = basis_ref[j]
        rows = weights_ref[pl.ds(pl.multiple_of(j * lines, lines), lines), :]
        weight = jnp.concatenate([rows[t : t + 1] for t in range(lines)], axis=1)
        weighted = (basis.astype(f32) * weight).astype(bf16)
        blocks.put_square(j, plan.covs, dot(weighted, basis, NT), units, 0)
        return jnp.where(column == j, dot(basis, work, NT), side)

    side = lax.fori_loop(0, plan.covs, diag_step, jnp.zeros(column.shape, f32))
    at = plan.covs * plan.tail
    side = jnp.concatenate([side, jnp.zeros((width, LANES - side.shape[1]), f32)], axis=1)
    blocks.put(plan.diag_blocks - 1, pltpu.roll(side, at, 1), units, 0, at, at + plan.covs)
    blocks.finish(mine_ref, theirs_ref)


def diag_sums(plan, core, weights, basis):
    work = pltpu.VMEM((up(plan.covs, 16), plan.bins), f32)
    return sums_call(
        plan, functools.partial(diag_kernel, plan), "diag_sums", plan.diag_units * UNIT, 10**9,
        [work], [smem(), vmem(), vmem()], core, weights, basis,
    )


def cross_kernel(plan, first, count, core_ref, pair_w_ref, left_ref, right_ref, mine_ref, theirs_ref, sums_ref):
    own, units = plan.own, plan.cross_units
    blocks = Blocks(plan, core_ref[0], sums_ref, count * units * UNIT)
    for m in range(count):
        blocks.clear(own, units, m * units * UNIT)

    def pair_step(i, carry):
        left, right = left_ref[i].astype(f32), right_ref[i]
        for m in range(count):
            start = (first + m) * plan.member
            turn = (LANES - (i % plan.rest_fold) * plan.rest) % LANES
            rest = pair_w_ref[pl.ds(start + own + i // plan.rest_fold, 1), :]
            rest = pltpu.roll(jnp.broadcast_to(rest, (8, LANES)), turn, 1)[:1, : plan.rest]
            weight = jnp.concatenate([pair_w_ref[pl.ds(start + i, 1), :], rest], axis=1)
            square = dot((left * weight).astype(bf16), right, NN)
            blocks.put_square(i, own, square, units, m * units * UNIT)
        return carry

    lax.fori_loop(0, own, pair_step, 0)
    blocks.finish(mine_ref, theirs_ref)


def cross_sums(plan, first, count, core, pair_w, left, right):
    return sums_call(
        plan, functools.partial(cross_kernel, plan, first, count), "cross_sums",
        count * plan.cross_units * UNIT, 10**9, [], [smem(), vmem(), vmem(), vmem()],
        core, pair_w, left, right,
    )


def add_kernel(*refs):
    out_ref = refs[-1]
    at = 0
    for mine_ref, got_ref in zip(refs[:-1:2], refs[1:-1:2]):
        rows = mine_ref.shape[0]
        out_ref[at : at + rows, :] = mine_ref[...] + got_ref[...]
        at += rows


def added(plan, parts):
    flat = [array for pair in parts for array in pair]
    rows = [array.shape[0] // plan.chips for array in flat]
    return pl.pallas_call(
        add_kernel,
        out_shape=jax.ShapeDtypeStruct((plan.chips * plan.share, LANES), f32),
        grid=(plan.chips,),
        in_specs=[pl.BlockSpec((r, LANES), lambda z: (z, 0)) for r in rows],
        out_specs=pl.BlockSpec((plan.share, LANES), lambda z: (z, 0)),
        compiler_params=params(),
        name="added",
        cost_estimate=pl.CostEstimate(flops=10**6, bytes_accessed=15 * 10**6, transcendentals=0),
    )(*flat)


def pack_kernel(plan, in_ref, out_ref):
    for k, (start, count) in enumerate(zip(plan.starts, plan.counts)):
        rows, steps = [], []
        for at in range(start, start + count, UNIT):
            part = in_ref[at : at + UNIT, :]
            top = jnp.max(jnp.max(jnp.abs(part), axis=0, keepdims=True), axis=1, keepdims=True)
            step = jnp.ceil(jnp.log2(jnp.maximum(top, 1e-30)) - 14.98)
            rows.append(jnp.round(part * jnp.exp2(-step)))
            steps.append(jnp.broadcast_to(step, (1, LANES)))
        steps.append(jnp.zeros((plan.chunk - count - len(steps), LANES), f32))
        out_ref[k] = jnp.concatenate(rows + steps, axis=0).astype(i32).astype(jnp.int16)


def packed(plan, share):
    return pl.pallas_call(
        functools.partial(pack_kernel, plan),
        out_shape=jax.ShapeDtypeStruct((plan.cluster + 1, plan.chunk, LANES), jnp.int16),
        in_specs=[vmem()],
        out_specs=vmem(),
        compiler_params=params(),
        name="packed",
        cost_estimate=pl.CostEstimate(flops=10**6, bytes_accessed=5 * 10**5, transcendentals=16),
    )(share)


def unpack_kernel(plan, each, core_ref, mine_ref, theirs_ref, cross_ref, diag_ref, side_ref, sums_ref):
    turn = pl.program_id(0)
    core = core_ref[0]
    width, covs = plan.width, plan.covs

    @pl.when(turn == 0)
    def _():
        def chip(z, carry):
            for ref, owner in ((mine_ref, 2 * z + core), (theirs_ref, 2 * z + 1 - core)):
                for k, (start, count) in enumerate(zip(plan.starts, plan.counts)):
                    part = ref[z, k * plan.chunk : (k + 1) * plan.chunk, :].astype(i32).astype(f32)
                    steps = jnp.exp2(part[count:])
                    for u in range(count // UNIT):
                        at = u * UNIT
                        sums_ref[owner, start + at : start + at + UNIT, :] = (
                            part[at : at + UNIT] * steps[u : u + 1]
                        )
            return carry

        lax.fori_loop(0, plan.chips, chip, 0)

    def block(b, units, base):
        pieces = []
        for cut in range(plan.cuts):
            unit = b * plan.cuts + cut
            row = pl.multiple_of(base + (unit % units) * UNIT, 8)
            pieces.append(sums_ref[unit // units, pl.ds(row, UNIT), :])
        return jnp.concatenate(pieces, axis=0)

    lane = lax.broadcasted_iota(i32, (width, LANES), 1)

    def square(ref, at, n, count, units, base):
        side = pltpu.roll(block(count + n // 2, units, base), (n % 2) * HALF, 1)
        tail = block(count + -(-count // 2), units, base)
        tail = pltpu.roll(tail, (HALF + LANES - n * plan.tail) % LANES, 1)
        ref[at, :, :LANES] = block(n, units, base)
        ref[at, :, LANES:] = jnp.where(lane < HALF, side, tail)[:, : width - LANES]

    def cross_step(k, carry):
        p = turn * each[0] + k
        base = (p // plan.own) * plan.cross_units * UNIT
        square(cross_ref, k, p % plan.own, plan.own, plan.cross_units, base)
        return carry

    def diag_step(k, carry):
        square(diag_ref, k, turn * each[1] + k, covs, plan.diag_units, plan.diag_at)
        return carry

    lax.fori_loop(0, each[0], cross_step, 0)
    lax.fori_loop(0, each[1], diag_step, 0)

    @pl.when(turn == 0)
    def _():
        at = covs * plan.tail
        last = block(plan.diag_blocks - 1, plan.diag_units, plan.diag_at)
        side_ref[...] = jnp.transpose(last)[at : at + covs]


def unpacked(plan, core, mine, theirs):
    width, pairs, covs = plan.width, plan.pairs, plan.covs
    turns = math.gcd(pairs, covs)
    each = (pairs // turns, covs // turns)
    return pl.pallas_call(
        functools.partial(unpack_kernel, plan, each),
        out_shape=(
            jax.ShapeDtypeStruct((pairs, width, width), f32),
            jax.ShapeDtypeStruct((covs, width, width), f32),
            jax.ShapeDtypeStruct((covs, width), f32),
        ),
        grid=(turns,),
        in_specs=[smem(), vmem(), vmem()],
        out_specs=(
            pl.BlockSpec((each[0], width, width), lambda p: (p, 0, 0)),
            pl.BlockSpec((each[1], width, width), lambda p: (p, 0, 0)),
            pl.BlockSpec((covs, width), lambda p: (0, 0)),
        ),
        scratch_shapes=[pltpu.VMEM((plan.devices, plan.share, LANES), f32)],
        compiler_params=params(),
        name="unpacked",
        cost_estimate=pl.CostEstimate(flops=10**6, bytes_accessed=17 * 10**6, transcendentals=0),
    )(core, mine, theirs)


def clusters_of(groups):
    side = math.isqrt(groups)
    if side * side == groups and side % 2 == 0:
        return [
            [(y + b) * side + x + a for b in range(2) for a in range(2)]
            for y in range(0, side, 2)
            for x in range(0, side, 2)
        ]
    return [[g] for g in range(groups)]


def place_in(clusters, group):
    table = [0] * sum(len(c) for c in clusters)
    for members in clusters:
        for place, g in enumerate(members):
            table[g] = place
    return jnp.asarray(table, i32)[group]


def on_device(
    bin_index, pair_bin, predictor, response, marginal_basis, pair_left, pair_right, pair_terms
):
    devices, groups = lax.axis_size("row"), lax.axis_size("grp")
    clusters = clusters_of(groups)
    cluster = len(clusters[0])
    covs, bins, width = marginal_basis.shape
    pairs, pair_block = pair_left.shape
    plan = Plan(devices, cluster, covs, width, bins, pairs, pair_block)
    rings = [list(range(c, devices, 2)) for c in range(2)]
    swap = [(d, d ^ 1) for d in range(devices)]
    me = lax.axis_index("row")
    core = (me % 2).astype(i32).reshape(1)
    place = place_in(clusters, lax.axis_index("grp"))
    basis = jnp.swapaxes(marginal_basis, 1, 2)

    mine, theirs = histograms(
        plan, core, jnp.transpose(bin_index), jnp.transpose(pair_bin),
        predictor.reshape(1, -1), response.reshape(1, -1),
    )
    sums = mine + lax.ppermute(theirs, "row", swap)
    sums = lax.psum_scatter(sums, "row", axis_index_groups=rings, tiled=True)

    def my_pairs(table):
        padded = jnp.pad(table, ((0, plan.padded - pairs), (0, 0)))
        return lax.dynamic_slice(padded, (place * plan.own, 0), (plan.own, table.shape[1]))

    def columns(table):
        blocks = my_pairs(table).reshape(plan.own, devices, plan.per)
        return jnp.transpose(blocks, (2, 1, 0)).reshape(pair_block, plan.own)

    terms = my_pairs(pair_terms)
    packets = picked_rows(plan, terms[:, 0], columns(pair_left), columns(pair_right % bins), basis)
    packets = lax.all_to_all(packets, "row", split_axis=0, concat_axis=0, tiled=True)

    left, right = ready_rows(plan, terms[:, 1], packets, basis)
    sums, left, right = lax.optimization_barrier((sums, left, right))
    pair_w = sums[plan.pair_at : plan.pair_at + cluster * plan.member]
    if cluster > 1:
        pair_w = lax.all_to_all(
            pair_w.reshape(cluster, plan.member, LANES), "grp", 0, 0,
            axis_index_groups=clusters, tiled=True,
        ).reshape(cluster * plan.member, LANES)
    diag = diag_sums(plan, core, sums, basis)
    step = -(-cluster // 2)
    parts = [
        cross_sums(plan, first, min(step, cluster - first), core, pair_w, left, right)
        for first in range(0, cluster, step)
    ] + [diag]
    total = added(plan, [(mine, lax.ppermute(theirs, "row", swap)) for mine, theirs in parts])
    total = lax.psum_scatter(total, "row", axis_index_groups=rings, tiled=True)
    chunks = packed(plan, total)
    if cluster > 1:
        cross = lax.all_to_all(
            chunks[:cluster], "grp", 0, 0, axis_index_groups=clusters, tiled=True
        )
        chunks = jnp.concatenate([cross, chunks[cluster:]], axis=0)
    length = chunks.shape[0] * plan.chunk
    mine = lax.all_gather(
        chunks.reshape(length, LANES), "row", axis=0, axis_index_groups=rings, tiled=True
    )
    theirs = lax.ppermute(mine, "row", swap)
    shape = (plan.chips, length, LANES)
    cross_blocks, diag_blocks, basis_response = unpacked(
        plan, core, mine.reshape(shape), theirs.reshape(shape)
    )
    return diag_blocks, cross_blocks, basis_response


def solution(mesh):
    return jax.shard_map(
        on_device,
        mesh=mesh,
        in_specs=(
            P(("grp", "row"), None),
            P(("grp", "row"), None),
            P(("grp", "row")),
            P(("grp", "row")),
            P(None, "row", None),
            P(None, "row"),
            P(None, "row"),
            P(),
        ),
        out_specs=(P("grp", None, None), P("grp", None, None), P("grp", None)),
        check_vma=False,
    )
```

```python
import functools
import math

import jax
import jax.numpy as jnp
from jax import lax
from jax.experimental import pallas as pl
from jax.experimental.pallas import tpu as pltpu
from jax.sharding import PartitionSpec as P

LANES = 128
HALF = 64
UNIT = 40
VMEM_LIMIT = 60 * 1024 * 1024
f32, bf16, i32 = jnp.float32, jnp.bfloat16, jnp.int32
NT = (((1,), (1,)), ((), ()))
NN = (((1,), (0,)), ((), ()))


def up(value, step):
    return -(-value // step) * step


def dot(a, b, dims):
    return lax.dot_general(a, b, dims, preferred_element_type=f32)


def vmem():
    return pl.BlockSpec(memory_space=pltpu.VMEM)


def smem():
    return pl.BlockSpec(memory_space=pltpu.SMEM)


def params():
    return pltpu.CompilerParams(vmem_limit_bytes=VMEM_LIMIT)


def two_terms(value):
    high = value.astype(bf16)
    return high, (value - high.astype(f32)).astype(bf16)


class Plan:
    def __init__(self, devices, cluster, covs, width, bins, pairs, pair_block):
        self.devices, self.cluster = devices, cluster
        self.covs, self.width, self.bins = covs, width, bins
        self.pairs, self.pair_block = pairs, pair_block
        self.chips = devices // 2
        self.per = pair_block // devices
        self.own = -(-pairs // cluster)
        self.padded = self.own * cluster
        self.parts = bins // 256
        self.work_at = covs * bins // LANES
        self.pair_at = 2 * self.work_at
        self.rest = pair_block - LANES
        self.rest_fold = LANES // self.rest
        self.member = up(self.own + -(-self.own // self.rest_fold), 8)
        self.sum_rows = up(self.pair_at + self.cluster * self.member, 8)
        self.slot = up(self.per * self.own, 16)
        self.tails = -(-self.slot // HALF)
        self.packet = self.slot + self.slot // 2 + 8 * self.tails
        self.cuts = width // UNIT
        self.tail = width - LANES - HALF
        self.cross_blocks = self.blocks_of(self.own)
        self.diag_blocks = self.blocks_of(covs)
        self.cross_units = -(-self.cross_blocks * self.cuts // devices)
        self.diag_units = -(-self.diag_blocks * self.cuts // devices)
        self.diag_at = cluster * self.cross_units * UNIT
        self.share = self.diag_at + self.diag_units * UNIT
        self.starts = [m * self.cross_units * UNIT for m in range(cluster)] + [self.diag_at]
        self.counts = [self.cross_units * UNIT] * cluster + [self.diag_units * UNIT]
        self.chunk = up(max(c + c // UNIT for c in self.counts), 16)

    def blocks_of(self, count):
        return count + -(-count // 2) + 1


def hist_kernel(plan, core_ref, bins_ref, pbins_ref, pred_ref, resp_ref, mine_ref, theirs_ref, iota_ref, own_ref, jo_ref):
    core = core_ref[0]
    rows = bins_ref.shape[1]
    iota_ref[...] = lax.broadcasted_iota(i32, iota_ref.shape, 0).astype(f32).astype(bf16)
    mine_ref[...] = jnp.zeros_like(mine_ref)
    theirs_ref[...] = jnp.zeros_like(theirs_ref)
    pred = pred_ref[...]
    rates = jnp.exp(pred)
    working = rates * pred + resp_ref[...] - rates
    rate_terms = two_terms(rates)
    work_terms = two_terms(working)
    chips, devices = plan.chips, plan.devices
    zero = jnp.zeros((), bf16)
    one = jnp.ones((), bf16)

    def place(owner):
        return ((owner & 1) ^ core) * chips + lax.shift_right_logical(owner, 1)

    def put(row, table):
        mine_ref[pl.ds(row, chips, stride=plan.sum_rows), :] = table[:chips]
        theirs_ref[pl.ds(row, chips, stride=plan.sum_rows), :] = table[chips:]

    middle = plan.pair_block // 2
    pair_bins = pbins_ref[...]
    fifth = jnp.floor((pair_bins.astype(f32) + 0.5) * (1.0 / plan.per)).astype(i32)
    holder = lax.shift_right_logical(fifth, devices.bit_length() - 1)
    within = (pair_bins - fifth * plan.per) * devices + holder
    late = (within >= middle).astype(i32)
    own_ref[...] = (place(fifth & (devices - 1)) + late * devices).astype(f32)
    jo_ref[...] = (within - late * middle).astype(f32)

    def pair_step(p, carry):
        own = own_ref[pl.ds(p, 1), :].astype(bf16)
        jo = jo_ref[pl.ds(p, 1), :].astype(bf16)
        own_hot = iota_ref[0 : 2 * devices, :] == own
        left = jnp.concatenate([jnp.where(own_hot, t, zero) for t in rate_terms], axis=0)
        right = jnp.where(iota_ref[0:middle, :] == jo, one, zero)
        both = dot(left, right, NT)
        table = both[: 2 * devices] + both[2 * devices :]
        table = jnp.concatenate([table, jnp.zeros((2 * devices, LANES - middle), f32)], axis=1)
        lane = lax.broadcasted_iota(i32, (devices, LANES), 1)
        second = table[devices:]
        first_line = plan.pair_at + (p // plan.own) * plan.member
        n = p % plan.own
        put(first_line + n, jnp.where(lane < middle, table[:devices], pltpu.roll(second, middle, 1)))
        line = first_line + plan.own + n // plan.rest_fold
        at = (n % plan.rest_fold) * plan.rest
        moved = pltpu.roll(second, (at + middle) % LANES, 1)
        keep = (lane[:chips] >= at) & (lane[:chips] < at + plan.rest)
        for ref, part in ((mine_ref, moved[:chips]), (theirs_ref, moved[chips:])):
            where = pl.ds(line, chips, stride=plan.sum_rows)
            ref[where, :] = jnp.where(keep, part, ref[where, :])
        return carry

    lax.fori_loop(0, plan.pairs, pair_step, 0, unroll=3)

    def cov_step(j, carry):
        ids = bins_ref[pl.ds(j, 1), :]
        owner = lax.shift_right_logical(ids, plan.bins.bit_length() - 1)
        offset = ids & (plan.bins - 1)
        spot = (lax.shift_right_logical(offset, 8) * devices + place(owner)).astype(f32).astype(bf16)
        low = (offset & 255).astype(f32).astype(bf16)
        spots = plan.parts * devices
        hot = iota_ref[0:spots, :] == spot
        left = jnp.concatenate([jnp.where(hot, t, zero) for t in rate_terms + work_terms], axis=0)
        right = jnp.where(iota_ref[0:256, :] == low, one, zero)
        both = dot(left, right, NT)
        for channel in range(2):
            base = 2 * channel * spots
            table = both[base : base + spots] + both[base + spots : base + 2 * spots]
            for part in range(plan.parts):
                for half in range(2):
                    put(
                        channel * plan.work_at + j * (plan.bins // LANES) + 2 * part + half,
                        table[part * devices : (part + 1) * devices, half * LANES : (half + 1) * LANES],
                    )
        return carry

    lax.fori_loop(0, plan.covs, cov_step, 0, unroll=2)


def histograms(plan, core, bins, pbins, pred, resp):
    rows = bins.shape[1]
    out = jax.ShapeDtypeStruct((plan.chips * plan.sum_rows, LANES), f32)
    tall = max(256, plan.parts * plan.devices)
    return pl.pallas_call(
        functools.partial(hist_kernel, plan),
        out_shape=(out, out),
        in_specs=[smem()] + [vmem()] * 4,
        out_specs=(vmem(), vmem()),
        scratch_shapes=[
            pltpu.VMEM((tall, rows), bf16),
            pltpu.VMEM(pbins.shape, f32),
            pltpu.VMEM(pbins.shape, f32),
        ],
        compiler_params=params(),
        name="histograms",
        cost_estimate=pl.CostEstimate(flops=12 * 10**9, bytes_accessed=8 * 10**6, transcendentals=rows),
    )(core, bins, pbins, pred, resp)


def pick_kernel(plan, terms_ref, left_ref, right_ref, basis_ref, out_ref, a_ref, b_ref):
    a_ref[...] = jnp.zeros_like(a_ref)
    b_ref[...] = jnp.zeros_like(b_ref)
    devices, slot = plan.devices, plan.slot
    count = plan.pair_block
    across = lax.broadcasted_iota(i32, (count, plan.bins), 1)
    lane = lax.broadcasted_iota(i32, (count, LANES), 1)
    extra = plan.width - LANES
    for i in range(plan.own):
        hot = (across == left_ref[:, i : i + 1]).astype(f32).astype(bf16)
        rows = dot(hot, basis_ref[terms_ref[i]], NT)
        right = right_ref[:, i : i + 1]
        high = lax.shift_right_logical(right, 5).astype(f32)
        low = (right & 31).astype(f32)
        end = jnp.concatenate([rows[:, LANES:], jnp.zeros((count, LANES - extra), f32)], axis=1)
        end = jnp.where(lane == extra, high, jnp.where(lane == extra + 1, low, end))
        for j in range(plan.per):
            where = pl.ds(j * plan.own + i, devices, stride=slot)
            a_ref[where, :] = rows[j * devices : (j + 1) * devices, :LANES]
            b_ref[where, :] = end[j * devices : (j + 1) * devices]

    def pack(q, carry):
        at = pl.multiple_of(q * slot, slot)
        a = a_ref[pl.ds(at, slot), :]
        b = b_ref[pl.ds(at, slot), :]
        half = slot // 2
        fold_lane = lax.broadcasted_iota(i32, (half, LANES), 1)
        folded = jnp.where(fold_lane < HALF, b[:half], pltpu.roll(b[half:], HALF, 1))
        tail_lane = lax.broadcasted_iota(i32, (8, LANES), 1)
        tails = []
        for n in range(plan.tails):
            tile = jnp.zeros((8, LANES), f32)
            for t in range(8):
                row = n * HALF + 8 * t
                if row >= slot:
                    break
                moved = pltpu.roll(b[row : row + 8], (16 * t - HALF) % LANES, 1)
                tile = jnp.where((tail_lane >= 16 * t) & (tail_lane < 16 * t + 16), moved, tile)
            tails.append(tile)
        out_ref[q] = jnp.concatenate([a, folded] + tails, axis=0).astype(bf16)
        return carry

    lax.fori_loop(0, devices, pack, 0)


def picked_rows(plan, terms, left, right, basis):
    return pl.pallas_call(
        functools.partial(pick_kernel, plan),
        out_shape=jax.ShapeDtypeStruct((plan.devices, plan.packet, LANES), bf16),
        in_specs=[smem()] + [vmem()] * 3,
        out_specs=vmem(),
        scratch_shapes=[pltpu.VMEM((plan.devices * plan.slot, LANES), f32)] * 2,
        compiler_params=params(),
        name="picked_rows",
        cost_estimate=pl.CostEstimate(flops=10**9, bytes_accessed=6 * 10**6, transcendentals=0),
    )(terms, left, right, basis)


class Blocks:
    def __init__(self, plan, core, sums_ref, share):
        self.plan, self.core, self.sums, self.share = plan, core, sums_ref, share

    def spot(self, block, cut, units, base):
        unit = block * self.plan.cuts + cut
        owner = unit // units
        place = ((owner & 1) ^ self.core) * self.plan.chips + lax.shift_right_logical(owner, 1)
        return pl.multiple_of(place * self.share + base + (unit % units) * UNIT, 8)

    def put(self, block, value, units, base, first=None, last=None):
        for cut in range(self.plan.cuts):
            where = pl.ds(self.spot(block, cut, units, base), UNIT)
            piece = value[cut * UNIT : (cut + 1) * UNIT]
            if first is not None:
                lane = lax.broadcasted_iota(i32, (UNIT, LANES), 1)
                keep = (lane >= first) & (lane < last)
                piece = jnp.where(keep, piece, self.sums[where, :])
            self.sums[where, :] = piece

    def put_square(self, n, count, square, units, base):
        width, tail = self.plan.width, self.plan.tail
        self.put(n, square[:, :LANES], units, base)
        rest = width - LANES
        side = jnp.concatenate([square[:, LANES:], jnp.zeros((width, LANES - rest), f32)], axis=1)
        at = (n % 2) * HALF
        self.put(count + n // 2, pltpu.roll(side, at, 1), units, base, at, at + HALF)
        at = n * tail
        moved = pltpu.roll(side, (at + HALF) % LANES, 1)
        self.put(count + -(-count // 2), moved, units, base, at, at + tail)

    def clear(self, count, units, base):
        plan = self.plan
        blocks = plan.blocks_of(count)
        parts = [(blocks - 1) * plan.cuts + c for c in range(plan.cuts)]
        parts += list(range(blocks * plan.cuts, units * plan.devices))
        if count % 2:
            parts += [(blocks - 2) * plan.cuts + c for c in range(plan.cuts)]
        for unit in parts:
            where = pl.ds(self.spot(unit // plan.cuts, unit % plan.cuts, units, base), UNIT)
            self.sums[where, :] = jnp.zeros((UNIT, LANES), f32)

    def finish(self, mine_ref, theirs_ref):
        half = self.plan.chips * self.share
        mine_ref[...] = self.sums[:half, :]
        theirs_ref[...] = self.sums[half:, :]


def sums_call(plan, kernel, name, share, flops, scratch, ins, *args):
    out = jax.ShapeDtypeStruct((plan.chips * share, LANES), f32)
    return pl.pallas_call(
        kernel,
        out_shape=(out, out),
        in_specs=ins,
        out_specs=(vmem(), vmem()),
        scratch_shapes=scratch + [pltpu.VMEM((2 * plan.chips * share, LANES), f32)],
        compiler_params=params(),
        name=name,
        cost_estimate=pl.CostEstimate(flops=flops, bytes_accessed=6 * 10**6, transcendentals=0),
    )(*args)


def ready_kernel(plan, terms_ref, packet_ref, basis_ref, left_ref, right_ref, a_ref, b_ref):
    devices, slot, own = plan.devices, plan.slot, plan.own
    half = slot // 2

    def unpack(o, carry):
        at = pl.multiple_of(o * slot, slot)
        y = packet_ref[o].astype(f32)
        a_ref[pl.ds(at, slot), :] = y[:slot]
        folded = y[slot : slot + half]
        turned = pltpu.roll(folded, HALF, 1)
        lane = lax.broadcasted_iota(i32, (8, LANES), 1)
        for n in range(plan.tails):
            tile = y[slot + half + 8 * n : slot + half + 8 * n + 8]
            for t in range(8):
                row = n * HALF + 8 * t
                if row >= slot:
                    break
                top = folded[row : row + 8] if row < half else turned[row - half : row - half + 8]
                moved = pltpu.roll(tile, (HALF - 16 * t) % LANES, 1)
                b_ref[pl.ds(at + row, 8), :] = jnp.where(lane < HALF, top, moved)
        return carry

    lax.fori_loop(0, devices, unpack, 0)
    across = lax.broadcasted_iota(i32, (plan.pair_block, plan.bins), 1)
    extra = plan.width - LANES

    def pair_step(i, carry):
        stride = [pl.ds(j * own + i, devices, stride=slot) for j in range(plan.per)]
        a = jnp.concatenate([a_ref[s, :] for s in stride], axis=0)
        b = jnp.concatenate([b_ref[s, :] for s in stride], axis=0)
        index = (b[:, extra : extra + 1] * 32.0 + b[:, extra + 1 : extra + 2]).astype(i32)
        hot = (across == index).astype(f32).astype(bf16)
        right_ref[i] = dot(hot, basis_ref[terms_ref[i]], NT).astype(bf16)
        left = jnp.concatenate([jnp.transpose(a), jnp.transpose(b)[:extra]], axis=0)
        left_ref[i] = left.astype(bf16)
        return carry

    lax.fori_loop(0, own, pair_step, 0)


def ready_rows(plan, terms, packets, basis):
    own, width, block = plan.own, plan.width, plan.pair_block
    return pl.pallas_call(
        functools.partial(ready_kernel, plan),
        out_shape=(
            jax.ShapeDtypeStruct((own, width, block), bf16),
            jax.ShapeDtypeStruct((own, block, width), bf16),
        ),
        in_specs=[smem(), vmem(), vmem()],
        out_specs=(vmem(), vmem()),
        scratch_shapes=[pltpu.VMEM((plan.devices * plan.slot, LANES), f32)] * 2,
        compiler_params=params(),
        name="ready_rows",
        cost_estimate=pl.CostEstimate(flops=10**9, bytes_accessed=7 * 10**6, transcendentals=0),
    )(terms, packets, basis)


def diag_part(plan, blocks, weights_ref, basis_ref, work_ref):
    width, units, base = plan.width, plan.diag_units, plan.diag_at
    blocks.clear(plan.covs, units, base)
    lines = plan.bins // LANES
    work_ref[...] = jnp.zeros_like(work_ref)
    for j in range(plan.covs):
        for t in range(lines):
            row = plan.work_at + j * lines + t
            work_ref[j : j + 1, t * LANES : (t + 1) * LANES] = weights_ref[row : row + 1, :]
    work = work_ref[...].astype(bf16)
    column = lax.broadcasted_iota(i32, (width, work_ref.shape[0]), 1)

    def diag_step(j, side):
        basis = basis_ref[j]
        rows = weights_ref[pl.ds(pl.multiple_of(j * lines, lines), lines), :]
        weight = jnp.concatenate([rows[t : t + 1] for t in range(lines)], axis=1)
        weighted = (basis.astype(f32) * weight).astype(bf16)
        blocks.put_square(j, plan.covs, dot(weighted, basis, NT), units, base)
        return jnp.where(column == j, dot(basis, work, NT), side)

    side = lax.fori_loop(0, plan.covs, diag_step, jnp.zeros(column.shape, f32))
    at = plan.covs * plan.tail
    side = jnp.concatenate([side, jnp.zeros((width, LANES - side.shape[1]), f32)], axis=1)
    blocks.put(plan.diag_blocks - 1, pltpu.roll(side, at, 1), units, base, at, at + plan.covs)


def cross_part(plan, blocks, pair_w_ref, left_ref, right_ref):
    own, units, count = plan.own, plan.cross_units, plan.cluster
    for m in range(count):
        blocks.clear(own, units, m * units * UNIT)

    def pair_step(i, carry):
        left, right = left_ref[i].astype(f32), right_ref[i]
        for m in range(count):
            start = m * plan.member
            turn = (LANES - (i % plan.rest_fold) * plan.rest) % LANES
            rest = pair_w_ref[pl.ds(start + own + i // plan.rest_fold, 1), :]
            rest = pltpu.roll(jnp.broadcast_to(rest, (8, LANES)), turn, 1)[:1, : plan.rest]
            weight = jnp.concatenate([pair_w_ref[pl.ds(start + i, 1), :], rest], axis=1)
            square = dot((left * weight).astype(bf16), right, NN)
            blocks.put_square(i, own, square, units, m * units * UNIT)
        return carry

    lax.fori_loop(0, own, pair_step, 0)


def products_kernel(plan, core_ref, weights_ref, pair_w_ref, left_ref, right_ref, basis_ref, mine_ref, theirs_ref, work_ref, sums_ref):
    blocks = Blocks(plan, core_ref[0], sums_ref, plan.share)
    diag_part(plan, blocks, weights_ref, basis_ref, work_ref)
    cross_part(plan, blocks, pair_w_ref, left_ref, right_ref)
    blocks.finish(mine_ref, theirs_ref)


def products(plan, core, weights, pair_w, left, right, basis):
    work = pltpu.VMEM((up(plan.covs, 16), plan.bins), f32)
    return sums_call(
        plan, functools.partial(products_kernel, plan), "products", plan.share, 3 * 10**9,
        [work], [smem()] + [vmem()] * 5, core, weights, pair_w, left, right, basis,
    )


def pack_kernel(plan, in_ref, out_ref):
    for k, (start, count) in enumerate(zip(plan.starts, plan.counts)):
        rows, steps = [], []
        for at in range(start, start + count, UNIT):
            part = in_ref[at : at + UNIT, :]
            top = jnp.max(jnp.max(jnp.abs(part), axis=0, keepdims=True), axis=1, keepdims=True)
            step = jnp.ceil(jnp.log2(jnp.maximum(top, 1e-30)) - 14.98)
            rows.append(jnp.round(part * jnp.exp2(-step)))
            steps.append(jnp.broadcast_to(step, (1, LANES)))
        steps.append(jnp.zeros((plan.chunk - count - len(steps), LANES), f32))
        out_ref[k] = jnp.concatenate(rows + steps, axis=0).astype(i32).astype(jnp.int16)


def packed(plan, share):
    return pl.pallas_call(
        functools.partial(pack_kernel, plan),
        out_shape=jax.ShapeDtypeStruct((plan.cluster + 1, plan.chunk, LANES), jnp.int16),
        in_specs=[vmem()],
        out_specs=vmem(),
        compiler_params=params(),
        name="packed",
        cost_estimate=pl.CostEstimate(flops=10**6, bytes_accessed=5 * 10**5, transcendentals=16),
    )(share)


def unpack_kernel(plan, each, core_ref, mine_ref, theirs_ref, cross_ref, diag_ref, side_ref, sums_ref):
    turn = pl.program_id(0)
    core = core_ref[0]
    width, covs = plan.width, plan.covs

    @pl.when(turn == 0)
    def _():
        def chip(z, carry):
            for ref, owner in ((mine_ref, 2 * z + core), (theirs_ref, 2 * z + 1 - core)):
                for k, (start, count) in enumerate(zip(plan.starts, plan.counts)):
                    part = ref[z, k * plan.chunk : (k + 1) * plan.chunk, :].astype(i32).astype(f32)
                    steps = jnp.exp2(part[count:])
                    for u in range(count // UNIT):
                        at = u * UNIT
                        sums_ref[owner, start + at : start + at + UNIT, :] = (
                            part[at : at + UNIT] * steps[u : u + 1]
                        )
            return carry

        lax.fori_loop(0, plan.chips, chip, 0)

    def block(b, units, base):
        pieces = []
        for cut in range(plan.cuts):
            unit = b * plan.cuts + cut
            row = pl.multiple_of(base + (unit % units) * UNIT, 8)
            pieces.append(sums_ref[unit // units, pl.ds(row, UNIT), :])
        return jnp.concatenate(pieces, axis=0)

    lane = lax.broadcasted_iota(i32, (width, LANES), 1)

    def square(ref, at, n, count, units, base):
        side = pltpu.roll(block(count + n // 2, units, base), (n % 2) * HALF, 1)
        tail = block(count + -(-count // 2), units, base)
        tail = pltpu.roll(tail, (HALF + LANES - n * plan.tail) % LANES, 1)
        ref[at, :, :LANES] = block(n, units, base)
        ref[at, :, LANES:] = jnp.where(lane < HALF, side, tail)[:, : width - LANES]

    def cross_step(k, carry):
        p = turn * each[0] + k
        base = (p // plan.own) * plan.cross_units * UNIT
        square(cross_ref, k, p % plan.own, plan.own, plan.cross_units, base)
        return carry

    def diag_step(k, carry):
        square(diag_ref, k, turn * each[1] + k, covs, plan.diag_units, plan.diag_at)
        return carry

    lax.fori_loop(0, each[0], cross_step, 0)
    lax.fori_loop(0, each[1], diag_step, 0)

    @pl.when(turn == 0)
    def _():
        at = covs * plan.tail
        last = block(plan.diag_blocks - 1, plan.diag_units, plan.diag_at)
        side_ref[...] = jnp.transpose(last)[at : at + covs]


def unpacked(plan, core, mine, theirs):
    width, pairs, covs = plan.width, plan.pairs, plan.covs
    turns = math.gcd(pairs, covs)
    each = (pairs // turns, covs // turns)
    return pl.pallas_call(
        functools.partial(unpack_kernel, plan, each),
        out_shape=(
            jax.ShapeDtypeStruct((pairs, width, width), f32),
            jax.ShapeDtypeStruct((covs, width, width), f32),
            jax.ShapeDtypeStruct((covs, width), f32),
        ),
        grid=(turns,),
        in_specs=[smem(), vmem(), vmem()],
        out_specs=(
            pl.BlockSpec((each[0], width, width), lambda p: (p, 0, 0)),
            pl.BlockSpec((each[1], width, width), lambda p: (p, 0, 0)),
            pl.BlockSpec((covs, width), lambda p: (0, 0)),
        ),
        scratch_shapes=[pltpu.VMEM((plan.devices, plan.share, LANES), f32)],
        compiler_params=params(),
        name="unpacked",
        cost_estimate=pl.CostEstimate(flops=10**6, bytes_accessed=17 * 10**6, transcendentals=0),
    )(core, mine, theirs)


def clusters_of(groups):
    side = math.isqrt(groups)
    if side * side == groups and side % 2 == 0:
        return [
            [(y + b) * side + x + a for b in range(2) for a in range(2)]
            for y in range(0, side, 2)
            for x in range(0, side, 2)
        ]
    return [[g] for g in range(groups)]


def place_in(clusters, group):
    table = [0] * sum(len(c) for c in clusters)
    for members in clusters:
        for place, g in enumerate(members):
            table[g] = place
    return jnp.asarray(table, i32)[group]


def on_device(
    bin_index, pair_bin, predictor, response, marginal_basis, pair_left, pair_right, pair_terms
):
    devices, groups = lax.axis_size("row"), lax.axis_size("grp")
    clusters = clusters_of(groups)
    cluster = len(clusters[0])
    covs, bins, width = marginal_basis.shape
    pairs, pair_block = pair_left.shape
    plan = Plan(devices, cluster, covs, width, bins, pairs, pair_block)
    rings = [list(range(c, devices, 2)) for c in range(2)]
    swap = [(d, d ^ 1) for d in range(devices)]
    me = lax.axis_index("row")
    core = (me % 2).astype(i32).reshape(1)
    place = place_in(clusters, lax.axis_index("grp"))
    basis = jnp.swapaxes(marginal_basis, 1, 2)

    mine, theirs = histograms(
        plan, core, jnp.transpose(bin_index), jnp.transpose(pair_bin),
        predictor.reshape(1, -1), response.reshape(1, -1),
    )
    sums = mine + lax.ppermute(theirs, "row", swap)
    sums = lax.psum_scatter(sums, "row", axis_index_groups=rings, tiled=True)

    def my_pairs(table):
        padded = jnp.pad(table, ((0, plan.padded - pairs), (0, 0)))
        return lax.dynamic_slice(padded, (place * plan.own, 0), (plan.own, table.shape[1]))

    def columns(table):
        blocks = my_pairs(table).reshape(plan.own, devices, plan.per)
        return jnp.transpose(blocks, (2, 1, 0)).reshape(pair_block, plan.own)

    terms = my_pairs(pair_terms)
    packets = picked_rows(plan, terms[:, 0], columns(pair_left), columns(pair_right % bins), basis)
    packets = lax.all_to_all(packets, "row", split_axis=0, concat_axis=0, tiled=True)

    left, right = ready_rows(plan, terms[:, 1], packets, basis)
    sums, left, right = lax.optimization_barrier((sums, left, right))
    pair_w = sums[plan.pair_at : plan.pair_at + cluster * plan.member]
    if cluster > 1:
        pair_w = lax.all_to_all(
            pair_w.reshape(cluster, plan.member, LANES), "grp", 0, 0,
            axis_index_groups=clusters, tiled=True,
        ).reshape(cluster * plan.member, LANES)
    mine, theirs = products(plan, core, sums, pair_w, left, right, basis)
    total = mine + lax.ppermute(theirs, "row", swap)
    total = lax.psum_scatter(total, "row", axis_index_groups=rings, tiled=True)
    chunks = packed(plan, total)
    if cluster > 1:
        cross = lax.all_to_all(
            chunks[:cluster], "grp", 0, 0, axis_index_groups=clusters, tiled=True
        )
        chunks = jnp.concatenate([cross, chunks[cluster:]], axis=0)
    length = chunks.shape[0] * plan.chunk
    mine = lax.all_gather(
        chunks.reshape(length, LANES), "row", axis=0, axis_index_groups=rings, tiled=True
    )
    theirs = lax.ppermute(mine, "row", swap)
    shape = (plan.chips, length, LANES)
    cross_blocks, diag_blocks, basis_response = unpacked(
        plan, core, mine.reshape(shape), theirs.reshape(shape)
    )
    return diag_blocks, cross_blocks, basis_response


def solution(mesh):
    return jax.shard_map(
        on_device,
        mesh=mesh,
        in_specs=(
            P(("grp", "row"), None),
            P(("grp", "row"), None),
            P(("grp", "row")),
            P(("grp", "row")),
            P(None, "row", None),
            P(None, "row"),
            P(None, "row"),
            P(),
        ),
        out_specs=(P("grp", None, None), P("grp", None, None), P("grp", None)),
        check_vma=False,
    )
```
